32 devices in a mesh: seq: 8 (over y, x, core), head: 4 (over z).
Axes of the slice: x: 2, y: 2, z: 4, core: 2. Of those that a mesh axis runs over, the one named last changes fastest.
Arguments:
- queries: bfloat16 [16384, 512], P('seq', 'head'), may hold values from -6 to 6
- keys: bfloat16 [16384, 512], P('seq', 'head'), may hold values from -6 to 6
- values: bfloat16 [16384, 512], P('seq', 'head'), may hold values from -6 to 6
- level_ids: int32 [16384], P('seq'), may hold values from 0 to 63
- level_table: float32 [64, 15], replicated, may hold values from 0 to 4, as said below
- out_cotangent: bfloat16 [16384, 2048], P('seq', 'head'), may hold values from -6 to 6
Outputs:
- attn_out: bfloat16 [16384, 512], P('seq', 'head')
- weight_grad: float32 [2048, 512], P('seq', 'head')
The draws below stay inside these ranges and needn't reach their ends.
Inputs may be any that keep to these rules, and one draw needn't show every extreme that they name: `level_table`: positive coefficients.
All inputs are finite; a program needn't handle non-finite values.
Results may differ from the reference program's by a relative error of at most 0.0043.
Values may be sent and summed in bfloat16 or wider, within the bound.
A program may use at most 64 MiB of HBM per device.

```python
import jax
import jax.numpy as jnp
from jax import lax

D = 2048
HD = 128
NID = 64
TOK_DEV = 2048
HEADS = 4
TOKENS = 16384
LOCAL_BITS = 11
SEQ_BITS = 3
LEVELS = 15
N_SEQ = 8


def draw_level_table(key, part):
    spread = jax.random.uniform(key, (NID, LEVELS), jnp.float32, -0.7, 0.7)
    level_depth = jnp.maximum(jnp.arange(LEVELS) - 1, 0).astype(jnp.float32)
    return jnp.exp(spread) * jnp.exp2(-0.5 * level_depth)[None, :]


def plant(entries, stream_key, low, largest):
    place = [jax.random.randint(jax.random.fold_in(stream_key, axis), (), 0, length) for axis, length in enumerate(entries.shape)]
    longest = entries.shape.index(max(entries.shape))
    next_to = place[:longest] + [(place[longest] + 1) % entries.shape[longest]] + place[longest + 1:]
    return entries.at[tuple(place)].set(low).at[tuple(next_to)].set(largest)


def with_spikes(values, key, source, target, blocks, factor):
    def block_of(dim):
        return (jnp.arange(values.shape[dim]) // (values.shape[dim] // blocks)).reshape((-1,) + (1,) * (values.ndim - 1 - dim))

    near = jax.random.permutation(key, blocks)[block_of(target)]
    second = (block_of(target) + blocks // 2) % blocks
    return jnp.where((block_of(source) == near) | (block_of(source) == second), factor * values, values)


def level_of(stream_key, dims, pieces, low, high):
    def one(dim, blocks):
        draws = jax.random.uniform(jax.random.fold_in(jax.random.fold_in(stream_key, 6), dim), (blocks,), jnp.float32, low / len(pieces), high / len(pieces))
        return jnp.repeat(jnp.exp(draws), dims[dim] // blocks).reshape((-1,) + (1,) * (len(dims) - dim - 1))

    factor_of = one(*pieces[0])
    for cut in pieces[1:]:
        factor_of = factor_of * one(*cut)
    return factor_of


def scatter_about(stream_key, dims, deviation, bound, cuts=(), kind=jnp.bfloat16):
    values = deviation * jax.random.normal(stream_key, dims, jnp.float32)
    if cuts:
        values = values * level_of(stream_key, dims, cuts, -0.22, 0.18)
    return jnp.clip(values, -bound, bound).astype(kind)


def bell_draw_with(rng, shape, width, most, split, heavy, held_as=jnp.bfloat16):
    result = width * jax.random.normal(rng, shape, jnp.float32)
    if split:
        result = result * level_of(rng, shape, split, -0.22, 0.18)
    return jnp.clip(with_spikes(result, jax.random.fold_in(rng, 3), *heavy), -most, most).astype(held_as)


def setup_inputs(seed: int = 0) -> dict:
    arg_keys = jax.random.split(jax.random.key(seed), 7)
    queries = scatter_about(arg_keys[0], (TOKENS, HEADS * HD), 1.0, 6.0, ((0, 8), (1, 4)))
    keys = scatter_about(arg_keys[1], (TOKENS, HEADS * HD), 1.0, 6.0, ((0, 8), (1, 4)))
    values = scatter_about(arg_keys[2], (TOKENS, HEADS * HD), 1.0, 6.0, ((0, 8), (1, 4)))
    level_ids = plant(jax.random.randint(arg_keys[3], (TOKENS,), 0, NID), jax.random.fold_in(arg_keys[3], 1), 0, NID - 1).astype(jnp.int32)
    level_table = draw_level_table(jax.random.fold_in(arg_keys[6], 71), 0)
    out_cotangent = bell_draw_with(arg_keys[5], (TOKENS, D), 1.0, 6.0, ((0, 8), (1, 4)), (0, 1, 8, 2.0))
    return dict(queries=queries, keys=keys, values=values, level_ids=level_ids, level_table=level_table, out_cotangent=out_cotangent)


EPSILON = 1e-06
HIGHEST = lax.Precision.HIGHEST

def level_index(row_pos, col_pos, bit_count):
    xor_value = jnp.bitwise_xor(row_pos, col_pos)
    levels = jnp.zeros(xor_value.shape, jnp.int32)
    for shift_by in range(bit_count):
        levels = levels + (jnp.right_shift(xor_value, shift_by) > 0).astype(jnp.int32)
    return levels

def split_heads(array):
    return array.reshape(N_SEQ, TOK_DEV, HEADS, HD).transpose(2, 0, 1, 3)

def reference(queries, keys, values, level_ids, level_table, out_cotangent):
    coeff = level_table[level_ids].reshape(N_SEQ, TOK_DEV, LEVELS)
    position = jnp.arange(TOK_DEV, dtype=jnp.int32)
    levels = level_index(position[:, None], position[None, :], LOCAL_BITS)
    causal = position[None, :] <= position[:, None]

    def block_weights(block_coeff):
        weights = jnp.zeros((TOK_DEV, TOK_DEV), jnp.float32)
        for level in range(LOCAL_BITS + 1):
            weights = weights + jnp.where(levels == level, block_coeff[:, level:level + 1], 0.0)
        return jnp.where(causal, weights, 0.0)
    all_weights = lax.map(block_weights, coeff)
    owner = jnp.arange(N_SEQ, dtype=jnp.int32)
    apart = jnp.bitwise_xor(owner[:, None], owner[None, :])
    earlier = owner[None, :] < owner[:, None]
    sibling = jnp.stack([((jnp.right_shift(apart, level) == 1) & earlier).astype(jnp.float32) for level in range(SEQ_BITS)])
    cross_coeff = coeff[:, :, LOCAL_BITS + 1:]

    def one_head(parts):
        query_blocks, key_blocks, value_blocks = parts

        def one_block(items):
            query, key_block, value, weights = items
            scores = jnp.dot(query, key_block.T, preferred_element_type=jnp.float32)
            mixed = (weights * scores).astype(jnp.bfloat16)
            local = jnp.dot(mixed, value, preferred_element_type=jnp.float32)
            state = jnp.dot(key_block.T, value, preferred_element_type=jnp.float32)
            return (local, state)
        local, states = lax.map(one_block, (query_blocks, key_blocks, value_blocks, all_weights))
        level_states = jnp.einsum('jcb,bde->jcde', sibling, states, precision=HIGHEST)
        readout = jnp.einsum('cti,jcie->ctje', query_blocks.astype(jnp.float32), level_states, precision=HIGHEST)
        cross = lax.optimization_barrier(jnp.sum(readout * cross_coeff[:, :, :, None], axis=2))
        total = local + cross
        normed = total * lax.rsqrt(lax.optimization_barrier(jnp.mean(total * total, axis=-1, keepdims=True)) + EPSILON)
        return normed.astype(jnp.bfloat16)
    heads_out = lax.map(one_head, (split_heads(queries), split_heads(keys), split_heads(values)))
    attn_out = heads_out.transpose(1, 2, 0, 3).reshape(TOKENS, HEADS * HD)
    weight_grad = jnp.dot(out_cotangent.T, attn_out, preferred_element_type=jnp.float32) * TOKENS ** (-0.5)
    return (attn_out, weight_grad)
```

```python
import functools

import jax
import jax.numpy as jnp
from jax import lax
from jax.experimental import pallas as pl
from jax.experimental.pallas import tpu as pltpu
from jax.sharding import PartitionSpec as P

EPSILON = 1e-06
TILE = 128
KEEP = 12
FIRST = 6
FILL = 8
EARLY = 2
AHEAD = 7
LAG = 4
MESH = pl.DeviceIdType.MESH
F32 = jnp.float32
BF16 = jnp.bfloat16


def dot(a, b, ca, cb):
    return lax.dot_general(a, b, (((ca,), (cb,)), ((), ())), preferred_element_type=F32)


def tile_levels(tile):
    row = lax.broadcasted_iota(jnp.int32, (tile, tile), 0)
    col = lax.broadcasted_iota(jnp.int32, (tile, tile), 1)
    apart = jnp.bitwise_xor(row, col)
    levels = jnp.zeros((tile, tile), jnp.int32)
    for bit in range(tile.bit_length() - 1):
        levels = levels + (jnp.right_shift(apart, bit) > 0).astype(jnp.int32)
    return jnp.where(col <= row, levels, -1)


def kept_tiles(n_head, tiles):
    return tiles * KEEP // 16 if n_head >= 4 else tiles


def kernel(
    n_seq, n_head,
    q_hbm, k_hbm, v_hbm, ids_ref, table_ref, cot_hbm,
    attn_hbm, grad_ref,
    q_ref, k_ref, v_ref, cot_ref, levels_ref, coeff_ref, total_ref, sib_ref,
    state_ref, states_ref, flat_ref, attn_ref, gather_ref, acc_ref,
    share_ref, shares_ref, final_ref, finals_ref, help_ref,
    load_sem, out_sem, state_send, state_recv, ring_send, ring_recv,
    share_send, share_recv, final_send, final_recv, help_send, help_recv,
):
    seq, head = lax.axis_index("seq"), lax.axis_index("head")
    block_len, head_dim = q_ref.shape
    width = cot_ref.shape[1]
    tiles = block_len // TILE
    pairs = tiles // 2
    tile_bits = TILE.bit_length() - 1
    local_bits = block_len.bit_length() - 1
    inner = local_bits - tile_bits
    seq_bits = n_seq.bit_length() - 1
    owners = n_seq // n_head
    rows_per = max(16, head_dim // n_seq)
    reducers = head_dim // rows_per
    piece = finals_ref.shape[2]
    last = n_head - 1
    keep = kept_tiles(n_head, tiles)
    helps = keep < tiles
    first, fill = min(FIRST, keep), min(FILL, keep)
    quads = tiles // 4
    early = min(EARLY, tiles)
    ahead = min(AHEAD, tiles)
    scale = (block_len * n_seq) ** (-0.5)

    loads = [
        pltpu.make_async_copy(src, dst, load_sem.at[i])
        for i, (src, dst) in enumerate(
            [(k_hbm, k_ref), (v_hbm, v_ref), (q_hbm, q_ref), (cot_hbm, cot_ref)]
        )
    ]
    for load in loads:
        load.start()

    barrier = pltpu.get_barrier_semaphore()
    me = seq * n_head + head

    def greet(step, carry):
        other = lax.rem(me + step, n_seq * n_head)
        pl.semaphore_signal(
            barrier, inc=1, device_id=(other // n_head, lax.rem(other, n_head)),
            device_id_type=MESH,
        )
        return carry

    lax.fori_loop(1, n_seq * n_head, greet, 0)

    table = table_ref[...]
    high = table.astype(BF16)
    rest = table - high.astype(F32)
    mid = rest.astype(BF16)
    low = (rest - mid.astype(F32)).astype(BF16)
    table3 = jnp.concatenate([high, mid, low], axis=1)
    levels_ref[...] = tile_levels(TILE)

    loads[0].wait()
    loads[1].wait()
    nodes = [
        dot(k_ref[pl.ds(i * TILE, TILE), :], v_ref[pl.ds(i * TILE, TILE), :], 0, 0)
        for i in range(tiles)
    ]
    for bit in range(inner):
        for i in range(tiles):
            place = (i >> bit) ^ 1
            value = nodes[place].astype(BF16) if (i >> bit) & 1 else jnp.zeros((head_dim, head_dim), BF16)
            sib_ref[i, :, pl.ds(bit * head_dim, head_dim)] = value
        nodes = [nodes[2 * i] + nodes[2 * i + 1] for i in range(len(nodes) // 2)]
    state_ref[...] = nodes[0].astype(BF16)

    loads[2].wait()

    def local_tile(i):
        rows = pl.ds(pl.multiple_of(i * TILE, TILE), TILE)
        row_ids = lax.broadcasted_iota(jnp.int32, (table.shape[1], TILE), 0)
        onehot = (row_ids == ids_ref[:, rows]).astype(F32).astype(BF16)
        coeff = dot(jnp.concatenate([onehot] * 3, axis=0), table3, 0, 1)
        coeff_ref[rows, :] = coeff
        levels = levels_ref[...]
        weights = jnp.zeros((TILE, TILE), F32)
        for level in range(tile_bits + 1):
            weights = jnp.where(levels == level, coeff[:, level : level + 1], weights)
        query = q_ref[rows, :]
        scores = dot(query, k_ref[rows, :], 1, 1)
        total = dot((weights * scores).astype(BF16), v_ref[rows, :], 1, 0)
        readout = dot(query, sib_ref[i], 1, 0)
        for bit in range(inner):
            level = tile_bits + 1 + bit
            total += coeff[:, level : level + 1] * readout[:, bit * head_dim : (bit + 1) * head_dim]
        total_ref[rows, :] = total

    def local_tiles(start, stop):
        def one(i, carry):
            local_tile(i)
            return carry

        lax.fori_loop(start, stop, one, 0, unroll=True)

    with jax.named_scope("local0"):
        local_tiles(0, early)

    with jax.named_scope("barrier"):
        pl.semaphore_wait(barrier, n_seq * n_head - 1)

    def state_copy(target):
        return pltpu.make_async_remote_copy(
            src_ref=state_ref, dst_ref=states_ref.at[seq],
            send_sem=state_send.at[0], recv_sem=state_recv.at[0],
            device_id=(target, head), device_id_type=MESH,
        )

    for target in range(1, n_seq):
        @pl.when(seq < target)
        def _():
            state_copy(target).start()

    right, left = lax.rem(head + 1, n_head), lax.rem(head + n_head - 1, n_head)
    neighbours = (right, left)
    places = (head, last - head)

    def origin_of(way, step):
        return step if way == 0 else last - step

    def help_copy(way, c):
        return pltpu.make_async_remote_copy(
            src_ref=cot_hbm.at[pl.ds(c * TILE, TILE), :],
            dst_ref=help_ref.at[pl.ds((c - keep) * TILE, TILE), :],
            send_sem=help_send.at[0], recv_sem=help_recv.at[c - keep],
            device_id=(seq, left if way == 0 else right), device_id_type=MESH,
        )

    def start_helps(begin, end):
        for way in range(2):
            @pl.when(places[way] == last)
            def _():
                for c in range(begin, end):
                    help_copy(way, c).start()

    if helps:
        start_helps(keep, keep + 1)

    with jax.named_scope("local1"):
        local_tiles(early, ahead)
    acc_ref[...] = jnp.zeros_like(acc_ref)

    with jax.named_scope("states"):
        for block in range(1, n_seq):
            @pl.when(seq == block)
            def _():
                arrived = states_ref.at[pl.ds(0, block)]
                pltpu.make_async_remote_copy(
                    src_ref=arrived, dst_ref=arrived,
                    send_sem=state_send.at[0], recv_sem=state_recv.at[0],
                    device_id=(0, head), device_id_type=MESH,
                ).wait_recv()

    for bit in range(seq_bits):
        span = 2**bit
        node = seq // span
        columns = pl.ds(bit * head_dim, head_dim)

        @pl.when(lax.rem(node, 2) == 1)
        def _():
            total = jnp.zeros((head_dim, head_dim), F32)
            for offset in range(span):
                total += states_ref[(node - 1) * span + offset].astype(F32)
            upper = total.astype(BF16)
            flat_ref[pl.ds(0, head_dim), columns] = upper
            flat_ref[pl.ds(head_dim, head_dim), columns] = (total - upper.astype(F32)).astype(BF16)

        @pl.when(lax.rem(node, 2) == 0)
        def _():
            flat_ref[:, columns] = jnp.zeros((2 * head_dim, head_dim), BF16)

    def ring_copy(way, origin, c):
        return pltpu.make_async_remote_copy(
            src_ref=gather_ref.at[origin, c], dst_ref=gather_ref.at[origin, c],
            send_sem=ring_send.at[way], recv_sem=ring_recv.at[origin, c],
            device_id=(seq, neighbours[way]), device_id_type=MESH,
        )

    def passes(way, c):
        place = places[way]
        return jnp.logical_or(place + 1 < last, jnp.logical_and(place < last, c < keep))

    def send_own(way, begin, end):
        def one(c, carry):
            ring_copy(way, head, c).start()
            return carry

        lax.fori_loop(begin, end, one, 0)

    def relay(way, step, c):
        place = places[way]
        origin = origin_of(way, step)
        ring_copy(way, origin, c).wait_recv()

        @pl.when(passes(way, c))
        def _():
            ring_copy(way, origin, c).start()

        if helps:
            mine = fill + step * (tiles - keep) + c - keep

            @pl.when(jnp.logical_and(jnp.logical_and(place == last - 1, c >= keep), mine < keep))
            def _():
                ring_copy(way, head, mine).start()

            if step == last - 2:
                @pl.when(jnp.logical_and(place == last - 1, c == tiles - 1))
                def _():
                    send_own(way, min(fill + (last - 1) * (tiles - keep), keep), keep)

        @pl.when(jnp.logical_and(jnp.logical_and(place == step + 1, place < (last - 1 if helps else last)), c == tiles - 1))
        def _():
            send_own(way, first, tiles)

    def attn_tile(i):
        rows = pl.ds(pl.multiple_of(i * TILE, TILE), TILE)
        query = q_ref[rows, :]
        readout = dot(jnp.concatenate([query, query], axis=1), flat_ref[...], 1, 0)
        coeff = coeff_ref[rows, :]
        cross = jnp.zeros((TILE, head_dim), F32)
        for bit in range(seq_bits):
            level = local_bits + 1 + bit
            cross += coeff[:, level : level + 1] * readout[:, bit * head_dim : (bit + 1) * head_dim]
        total = total_ref[rows, :] + cross
        normed = total * lax.rsqrt(jnp.mean(total * total, axis=1, keepdims=True) + EPSILON)
        attn_ref[rows, :] = normed.astype(BF16)
        gather_ref[head, i] = normed.T.astype(BF16)

    lags = [jnp.minimum(LAG * place, pairs) for place in places]

    def sooner(way):
        return jnp.where(places[way] == last - 1, fill, first) if helps else first

    def middle(way):
        return jnp.logical_and(places[way] >= 1, places[way] < last)

    def produce(local):
        def step(t, carry):
            attn_tile(t)
            if local:
                local_tile(t + ahead)
            for way in range(2):
                @pl.when(jnp.logical_and(passes(way, t), jnp.logical_or(places[way] == 0, t < sooner(way))))
                def _():
                    ring_copy(way, head, t).start()
            for way in range(2):
                @pl.when(jnp.logical_and(middle(way), t >= lags[way]))
                def _():
                    relay(way, 0, t - lags[way])
            return carry
        return step

    with jax.named_scope("phase1a"):
        lax.fori_loop(0, tiles - ahead, produce(True), 0)
    with jax.named_scope("phase1b"):
        lax.fori_loop(tiles - ahead, tiles, produce(False), 0)
    if helps:
        start_helps(keep + 1, tiles)

    attn_copy = pltpu.make_async_copy(attn_ref, attn_hbm, out_sem.at[0])
    attn_copy.start()

    def joined(origin, q):
        return jnp.concatenate([gather_ref[origin, 4 * q + i] for i in range(4)], axis=1)

    def multiply(origin, q):
        rows = pl.ds(pl.multiple_of(q * (4 * TILE), 4 * TILE), 4 * TILE)
        acc_ref[origin] += dot(joined(origin, q), cot_ref[rows, :], 1, 0)

    def multiply_help(origin, q):
        rows = pl.ds(pl.multiple_of((q - keep // 4) * (4 * TILE), 4 * TILE), 4 * TILE)
        acc_ref[n_head + origin] += dot(joined(origin, q), help_ref[rows, :], 1, 0)

    def share_copy(slot, target):
        return pltpu.make_async_remote_copy(
            src_ref=share_ref.at[slot, pl.ds(target * rows_per, rows_per), :],
            dst_ref=shares_ref.at[slot, lax.rem(seq - target + n_seq, n_seq) - 1],
            send_sem=share_send.at[slot], recv_sem=share_recv.at[slot],
            device_id=(target, head), device_id_type=MESH,
        )

    def send_share(slot):
        share_ref[slot] = (acc_ref[slot] * scale).astype(BF16)
        for target in range(reducers):
            @pl.when(seq != target)
            def _():
                share_copy(slot, target).start()

    def final_copy(slot, block, origin, kind, owner):
        columns = pl.ds(owner * piece if piece < width else 0, piece)
        return pltpu.make_async_remote_copy(
            src_ref=final_ref.at[slot, :, columns] if piece < width else final_ref.at[slot],
            dst_ref=finals_ref.at[kind, pl.ds(pl.multiple_of(seq * rows_per, rows_per), rows_per), :],
            send_sem=final_send.at[slot], recv_sem=final_recv.at[kind],
            device_id=(block * owners + owner, origin), device_id_type=MESH,
        )

    def is_self(block, origin, owner):
        return jnp.logical_and(block * owners + owner == seq, origin == head)

    def reduce_share(slot, block, origin, kind):
        @pl.when(seq < reducers)
        def _():
            mine = pl.ds(pl.multiple_of(seq * rows_per, rows_per), rows_per)
            arrived = shares_ref.at[slot]
            pltpu.make_async_remote_copy(
                src_ref=arrived, dst_ref=arrived,
                send_sem=share_send.at[slot], recv_sem=share_recv.at[slot],
                device_id=(0, head), device_id_type=MESH,
            ).wait_recv()
            whole = acc_ref[slot, mine, :] * scale
            for source in range(n_seq - 1):
                whole += shares_ref[slot, source].astype(F32)
            final_ref[slot] = whole
            for owner in range(owners):
                @pl.when(jnp.logical_not(is_self(block, origin, owner)))
                def _():
                    final_copy(slot, block, origin, kind, owner).start()

                @pl.when(is_self(block, origin, owner))
                def _():
                    start = owner * piece if piece < width else 0
                    finals_ref[kind, mine, :] = final_ref[slot, :, pl.ds(start, piece)]

    loads[3].wait()

    def kept_quad(way, q):
        return jnp.logical_or(places[way] < last, 4 * q < keep)

    def arrive(way, step, q):
        for c in range(4):
            ring_copy(way, origin_of(way, step), 4 * q + c).wait_recv()

    def settle(u, carry):
        for way in range(2):
            c = tiles + u - lags[way]

            @pl.when(jnp.logical_and(middle(way), c < tiles))
            def _():
                relay(way, 0, c)
        q = u // 2

        @pl.when(lax.rem(u, 2) == 0)
        def _():
            multiply(head, q)

        @pl.when(lax.rem(u, 2) == 1)
        def _():
            for way in range(2):
                @pl.when(jnp.logical_and(places[way] > 0, kept_quad(way, q)))
                def _():
                    pl.when(places[way] == last)(lambda: arrive(way, 0, q))
                    multiply(origin_of(way, 0), q)
        return carry

    with jax.named_scope("settle"):
        lax.fori_loop(0, 2 * quads, settle, 0)

    def send_all(group):
        for condition, slot, _, _, _ in group:
            pl.when(condition)(functools.partial(send_share, slot))

    def reduce_all(group):
        for condition, *rest in group:
            pl.when(condition)(functools.partial(reduce_share, *rest))

    waiting = [(head >= 0, head, head, head, 0)]
    for way in range(2):
        waiting.append((places[way] > 0, origin_of(way, 0), head, origin_of(way, 0), 0))
    with jax.named_scope("share0"):
        send_all(waiting)
    if last > 1:
        nearest = []
        for way in range(2):
            origin = origin_of(way, last - 1)
            nearest.append((places[way] == last, origin, head, origin, 0))

            def near(q, carry):
                arrive(way, last - 1, q)
                multiply(origin, q)
                return carry

            @pl.when(places[way] == last)
            def _():
                with jax.named_scope("near"):
                    lax.fori_loop(0, keep // 4, near, 0)
                    send_share(origin)
        waiting += nearest
    every = list(waiting)

    for step in range(1, last - 1):
        helped = []
        if helps and step == 1:
            for way in range(2):
                for origin in (head, origin_of(way, 0)):
                    block = last if way == 0 else 0
                    helped.append((places[way] == last - 1, n_head + origin, block, origin, 1))

        def stream(q, carry):
            for i in range(4):
                c = 4 * q + i
                for way in range(2):
                    place = places[way]

                    @pl.when(jnp.logical_and(place > step, place < last))
                    def _():
                        relay(way, step, c)
            for way in range(2):
                place, origin = places[way], origin_of(way, step)

                @pl.when(jnp.logical_and(place > step, kept_quad(way, q)))
                def _():
                    pl.when(place == last)(lambda: arrive(way, step, q))
                    multiply(origin, q)

                if helps:
                    @pl.when(jnp.logical_and(place == last - 1, 4 * q >= keep))
                    def _():
                        multiply_help(origin, q)
            if helps and step == 1:
                for way in range(2):
                    @pl.when(jnp.logical_and(places[way] == last - 1, q == quads - 2))
                    def _():
                        for c in range(keep, tiles):
                            help_copy(way, c).wait_recv()
                        for group in range(keep // 4, quads):
                            multiply_help(head, group)
                            multiply_help(origin_of(way, 0), group)
                        send_share(n_head + head)
                        send_share(n_head + origin_of(way, 0))

            @pl.when(q == quads - 2)
            def _():
                reduce_all(waiting)
            return carry

        with jax.named_scope("stream%d" % step):
            lax.fori_loop(0, quads, stream, 0)

        done = []
        for way in range(2):
            place, origin = places[way], origin_of(way, step)
            done.append((place > step, origin, head, origin, 0))
            if helps:
                block = last if way == 0 else 0
                done.append((place == last - 1, n_head + origin, block, origin, 1))
        with jax.named_scope("share%d" % step):
            send_all(done)
        every += helped + done
        waiting = helped + done
    with jax.named_scope("reducelast"):
        reduce_all(waiting)

    with jax.named_scope("finals"):
        home = seq // owners
        at_end = jnp.logical_and(jnp.logical_or(home == 0, home == last), head != home)
        for kind in range(2 if helps else 1):
            plane = home if kind == 0 else jnp.where(home == 0, 1, last - 1)
            own = jnp.logical_and(seq < reducers, head == plane)
            expected = at_end if kind else seq >= 0
            for count, match in ((reducers - 1, own), (reducers, jnp.logical_not(own))):
                @pl.when(jnp.logical_and(expected, match))
                def _():
                    arrived = finals_ref.at[kind, pl.ds(0, count * rows_per), :]
                    pltpu.make_async_remote_copy(
                        src_ref=arrived, dst_ref=arrived,
                        send_sem=final_send.at[0], recv_sem=final_recv.at[kind],
                        device_id=(0, plane), device_id_type=MESH,
                    ).wait_recv()
        if helps:
            @pl.when(at_end)
            def _():
                finals_ref[0] += finals_ref[1]
        per = grad_ref.shape[1]
        if per == piece:
            grad_ref[...] = finals_ref[0]
        else:
            for owner in range(owners):
                @pl.when(lax.rem(seq, owners) == owner)
                def _():
                    grad_ref[...] = finals_ref[0][:, owner * per : (owner + 1) * per]

    with jax.named_scope("drain"):
        for block in range(n_seq - 1):
            @pl.when(seq == block)
            def _():
                sent = states_ref.at[pl.ds(0, n_seq - 1 - block)]
                pltpu.make_async_remote_copy(
                    src_ref=sent, dst_ref=sent,
                    send_sem=state_send.at[0], recv_sem=state_recv.at[0],
                    device_id=(0, head), device_id_type=MESH,
                ).wait_send()
        for way in range(2):
            if helps:
                @pl.when(places[way] == last)
                def _():
                    pltpu.make_async_remote_copy(
                        src_ref=help_ref, dst_ref=help_ref,
                        send_sem=help_send.at[0], recv_sem=help_recv.at[0],
                        device_id=(seq, left if way == 0 else right), device_id_type=MESH,
                    ).wait_send()
            for place in range(last):
                @pl.when(places[way] == place)
                def _():
                    count = tiles if place + 1 < last else keep
                    sent = gather_ref.at[pl.ds(0, place + 1), pl.ds(0, count)]
                    pltpu.make_async_remote_copy(
                        src_ref=sent, dst_ref=sent,
                        send_sem=ring_send.at[way], recv_sem=ring_recv.at[0, 0],
                        device_id=(seq, neighbours[way]), device_id_type=MESH,
                    ).wait_send()
        for condition, slot, block, origin, kind in every:
            @pl.when(condition)
            def _():
                def sent_shares(count):
                    sent = share_ref.at[slot, pl.ds(0, count * rows_per), :]
                    pltpu.make_async_remote_copy(
                        src_ref=sent, dst_ref=sent,
                        send_sem=share_send.at[slot], recv_sem=share_recv.at[slot],
                        device_id=(0, head), device_id_type=MESH,
                    ).wait_send()

                def sent_finals(count):
                    sent = finals_ref.at[0, pl.ds(0, count * rows_per), :]
                    pltpu.make_async_remote_copy(
                        src_ref=sent, dst_ref=sent,
                        send_sem=final_send.at[slot], recv_sem=final_recv.at[0],
                        device_id=(0, head), device_id_type=MESH,
                    ).wait_send()

                pl.when(seq < reducers)(lambda: sent_shares(reducers - 1))
                if reducers < n_seq:
                    pl.when(seq >= reducers)(lambda: sent_shares(reducers))
                near = jnp.logical_and(seq // owners == block, origin == head)
                pl.when(jnp.logical_and(seq < reducers, jnp.logical_not(near)))(lambda: sent_finals(owners))
                if owners > 1:
                    pl.when(jnp.logical_and(seq < reducers, near))(lambda: sent_finals(owners - 1))
        attn_copy.wait()


def finish(attn_ref, grad_ref, attn_out, grad_out, held_ref, sem):
    rows = attn_ref.shape[0] // 4
    parts = [pl.ds(i * rows, rows) for i in range(4)]
    takes = [pltpu.make_async_copy(attn_ref.at[part], held_ref.at[part], sem.at[0, i]) for i, part in enumerate(parts)]
    puts = [pltpu.make_async_copy(held_ref.at[part], attn_out.at[part], sem.at[1, i]) for i, part in enumerate(parts)]
    for take in takes:
        take.start()
    grad_out[...] = grad_ref[...].T
    for take, put in zip(takes, puts):
        take.wait()
        put.start()
    for put in puts:
        put.wait()


def body(n_seq, n_head, queries, keys, values, level_ids, level_table, out_cotangent):
    block_len, head_dim = queries.shape
    width = out_cotangent.shape[1]
    per = width * n_head // n_seq
    piece = per if per % 128 == 0 else width
    seq_bits = n_seq.bit_length() - 1
    tiles = block_len // TILE
    inner = tiles.bit_length() - 1
    rows_per = max(16, head_dim // n_seq)
    slots = 2 * n_head
    spare = max(1, tiles - kept_tiles(n_head, tiles))
    dma = pltpu.SemaphoreType.DMA
    vmem = pl.BlockSpec(memory_space=pltpu.VMEM)
    hbm = pl.BlockSpec(memory_space=pl.ANY)
    attn_out, grad = pl.pallas_call(
        functools.partial(kernel, n_seq, n_head),
        out_shape=(
            jax.ShapeDtypeStruct((block_len, head_dim), BF16),
            jax.ShapeDtypeStruct((head_dim, per), F32),
        ),
        in_specs=[hbm, hbm, hbm, vmem, vmem, hbm],
        out_specs=(hbm, vmem),
        scratch_shapes=[
            pltpu.VMEM((block_len, head_dim), BF16),
            pltpu.VMEM((block_len, head_dim), BF16),
            pltpu.VMEM((block_len, head_dim), BF16),
            pltpu.VMEM((block_len, width), BF16),
            pltpu.VMEM((TILE, TILE), jnp.int32),
            pltpu.VMEM((block_len, level_table.shape[1]), F32),
            pltpu.VMEM((block_len, head_dim), F32),
            pltpu.VMEM((tiles, head_dim, inner * head_dim), BF16),
            pltpu.VMEM((head_dim, head_dim), BF16),
            pltpu.VMEM((n_seq, head_dim, head_dim), BF16),
            pltpu.VMEM((2 * head_dim, seq_bits * head_dim), BF16),
            pltpu.VMEM((block_len, head_dim), BF16),
            pltpu.VMEM((n_head, tiles, head_dim, TILE), BF16),
            pltpu.VMEM((slots, head_dim, width), F32),
            pltpu.VMEM((slots, head_dim, width), BF16),
            pltpu.VMEM((slots, n_seq - 1, rows_per, width), BF16),
            pltpu.VMEM((slots, rows_per, width), F32),
            pltpu.VMEM((2, head_dim, piece), F32),
            pltpu.VMEM((spare * TILE, width), BF16),
            dma((4,)),
            dma((1,)),
            dma((1,)),
            dma((1,)),
            dma((2,)),
            dma((n_head, tiles)),
            dma((slots,)),
            dma((slots,)),
            dma((slots,)),
            dma((2,)),
            dma((1,)),
            dma((spare,)),
        ],
        compiler_params=pltpu.CompilerParams(
            collective_id=0, has_side_effects=True, vmem_limit_bytes=60 * 2**20
        ),
    )(queries, keys, values, level_ids[None, :], level_table.T, out_cotangent)
    return pl.pallas_call(
        finish,
        out_shape=(
            jax.ShapeDtypeStruct((block_len, head_dim), BF16),
            jax.ShapeDtypeStruct((per, head_dim), F32),
        ),
        in_specs=[hbm, vmem],
        out_specs=(hbm, vmem),
        scratch_shapes=[pltpu.VMEM((block_len, head_dim), BF16), dma((2, 4))],
    )(attn_out, grad)


def solution(mesh):
    in_specs = (
        P("seq", "head"),
        P("seq", "head"),
        P("seq", "head"),
        P("seq"),
        P(),
        P("seq", "head"),
    )
    out_specs = (P("seq", "head"), P("seq", "head"))
    return jax.shard_map(
        functools.partial(body, mesh.shape["seq"], mesh.shape["head"]),
        mesh=mesh, in_specs=in_specs, out_specs=out_specs, check_vma=False,
    )
```

```python
import functools

import jax
import jax.numpy as jnp
from jax import lax
from jax.experimental import pallas as pl
from jax.experimental.pallas import tpu as pltpu
from jax.sharding import PartitionSpec as P

EPSILON = 1e-06
TILE = 128
KEEP = 12
EARLY = 2
AHEAD = 10
LAG = 4
BURST = 2
MESH = pl.DeviceIdType.MESH
F32 = jnp.float32
BF16 = jnp.bfloat16


def dot(a, b, ca, cb):
    return lax.dot_general(a, b, (((ca,), (cb,)), ((), ())), preferred_element_type=F32)


def tile_levels(tile):
    row = lax.broadcasted_iota(jnp.int32, (tile, tile), 0)
    col = lax.broadcasted_iota(jnp.int32, (tile, tile), 1)
    apart = jnp.bitwise_xor(row, col)
    levels = jnp.zeros((tile, tile), jnp.int32)
    for bit in range(tile.bit_length() - 1):
        levels = levels + (jnp.right_shift(apart, bit) > 0).astype(jnp.int32)
    return jnp.where(col <= row, levels, -1)


def kept_tiles(n_head, tiles):
    return tiles * KEEP // 16 if n_head >= 4 else tiles


def kernel(
    n_seq, n_head,
    q_hbm, k_hbm, v_hbm, ids_hbm, table_hbm, cot_hbm,
    attn_ref, grad_ref,
    q_ref, k_ref, v_ref, cot_ref, ids_ref, table_ref, levels_ref, coeff_ref, total_ref, sib_ref,
    state_ref, states_ref, flat_ref, gather_ref, acc_ref,
    share_ref, shares_ref, final_ref, finals_ref, help_ref,
    load_sem, state_send, state_recv, ring_send, ring_recv,
    share_send, share_recv, final_send, final_recv, help_send, help_recv,
):
    seq, head = lax.axis_index("seq"), lax.axis_index("head")
    block_len, head_dim = q_ref.shape
    width = cot_ref.shape[1]
    tiles = block_len // TILE
    pairs = tiles // 2
    tile_bits = TILE.bit_length() - 1
    local_bits = block_len.bit_length() - 1
    inner = local_bits - tile_bits
    seq_bits = n_seq.bit_length() - 1
    owners = n_seq // n_head
    rows_per = max(16, head_dim // n_seq)
    reducers = head_dim // rows_per
    piece = finals_ref.shape[2]
    last = n_head - 1
    keep = kept_tiles(n_head, tiles)
    helps = keep < tiles
    quads = tiles // 4
    early = min(EARLY, tiles)
    ahead = min(AHEAD, tiles)
    scale = (block_len * n_seq) ** (-0.5)

    loads = [
        pltpu.make_async_copy(src, dst, load_sem.at[i])
        for i, (src, dst) in enumerate(
            [
                (k_hbm, k_ref), (v_hbm, v_ref), (table_hbm, table_ref), (ids_hbm, ids_ref),
                (q_hbm, q_ref), (cot_hbm, cot_ref),
            ]
        )
    ]
    for load in loads:
        load.start()

    barrier = pltpu.get_barrier_semaphore()

    def greet(device):
        pl.semaphore_signal(barrier, inc=1, device_id=device, device_id_type=MESH)

    for step in range(1, n_seq):
        greet((lax.rem(seq + step, n_seq), head))
    pl.when(head > 0)(lambda: greet((seq, head - 1)))
    pl.when(head < n_head - 1)(lambda: greet((seq, head + 1)))

    levels_ref[...] = tile_levels(TILE)
    for load in loads[:4]:
        load.wait()
    table = table_ref[...]
    high = table.astype(BF16)
    rest = table - high.astype(F32)
    mid = rest.astype(BF16)
    low = (rest - mid.astype(F32)).astype(BF16)
    table3 = jnp.concatenate([high, mid, low], axis=1)

    nodes = [
        dot(k_ref[pl.ds(i * TILE, TILE), :], v_ref[pl.ds(i * TILE, TILE), :], 0, 0)
        for i in range(tiles)
    ]
    for bit in range(inner):
        for i in range(tiles):
            place = (i >> bit) ^ 1
            value = nodes[place].astype(BF16) if (i >> bit) & 1 else jnp.zeros((head_dim, head_dim), BF16)
            sib_ref[i, :, pl.ds(bit * head_dim, head_dim)] = value
        nodes = [nodes[2 * i] + nodes[2 * i + 1] for i in range(len(nodes) // 2)]
    state_ref[...] = nodes[0].astype(BF16)

    loads[4].wait()

    def local_tile(i):
        rows = pl.ds(pl.multiple_of(i * TILE, TILE), TILE)
        row_ids = lax.broadcasted_iota(jnp.int32, (table.shape[1], TILE), 0)
        onehot = (row_ids == ids_ref[:, rows]).astype(F32).astype(BF16)
        coeff = dot(jnp.concatenate([onehot] * 3, axis=0), table3, 0, 1)
        coeff_ref[rows, :] = coeff
        levels = levels_ref[...]
        weights = jnp.zeros((TILE, TILE), F32)
        for level in range(tile_bits + 1):
            weights = jnp.where(levels == level, coeff[:, level : level + 1], weights)
        query = q_ref[rows, :]
        scores = dot(query, k_ref[rows, :], 1, 1)
        total = dot((weights * scores).astype(BF16), v_ref[rows, :], 1, 0)
        readout = dot(query, sib_ref[i], 1, 0)
        for bit in range(inner):
            level = tile_bits + 1 + bit
            total += coeff[:, level : level + 1] * readout[:, bit * head_dim : (bit + 1) * head_dim]
        total_ref[rows, :] = total

    def local_tiles(start, stop):
        def one(i, carry):
            local_tile(jnp.where(head < n_head // 2, i, tiles - 1 - i))
            return carry

        lax.fori_loop(start, stop, one, 0, unroll=True)

    with jax.named_scope("local0"):
        local_tiles(0, early)

    with jax.named_scope("barrier"):
        pl.semaphore_wait(barrier, n_seq - 1 + jnp.minimum(head, 1) + jnp.minimum(last - head, 1))

    def state_copy(target):
        return pltpu.make_async_remote_copy(
            src_ref=state_ref, dst_ref=states_ref.at[seq],
            send_sem=state_send.at[0], recv_sem=state_recv.at[0],
            device_id=(target, head), device_id_type=MESH,
        )

    for target in range(1, n_seq):
        @pl.when(seq < target)
        def _():
            state_copy(target).start()

    right, left = lax.rem(head + 1, n_head), lax.rem(head + n_head - 1, n_head)
    neighbours = (right, left)
    places = (head, last - head)

    half = n_head // 2
    spare = tiles - keep

    def origin_of(way, distance):
        return head - distance if way == 0 else head + distance

    def tile_of(origin, i):
        return jnp.where(origin < half, i, tiles - 1 - i)

    def quad_of(origin, j):
        return jnp.where(origin < half, j, quads - 1 - j)

    def kept(way, c):
        return c >= spare if way == 0 else c < keep

    def kept_quad(way, q):
        return 4 * q >= spare if way == 0 else 4 * q < keep

    def help_copy(way, i):
        return pltpu.make_async_remote_copy(
            src_ref=cot_hbm.at[pl.ds(i * TILE if way == 0 else (keep + i) * TILE, TILE), :],
            dst_ref=help_ref.at[pl.ds(i * TILE, TILE), :],
            send_sem=help_send.at[0], recv_sem=help_recv.at[i],
            device_id=(seq, left if way == 0 else right), device_id_type=MESH,
        )

    for way in range(2):
        @pl.when(places[way] == last)
        def _():
            for i in range(spare):
                help_copy(way, i).start()

    with jax.named_scope("local1"):
        local_tiles(early, ahead)
    acc_ref[...] = jnp.zeros_like(acc_ref)

    with jax.named_scope("states"):
        for block in range(1, n_seq):
            @pl.when(seq == block)
            def _():
                arrived = states_ref.at[pl.ds(0, block)]
                pltpu.make_async_remote_copy(
                    src_ref=arrived, dst_ref=arrived,
                    send_sem=state_send.at[0], recv_sem=state_recv.at[0],
                    device_id=(0, head), device_id_type=MESH,
                ).wait_recv()

    for bit in range(seq_bits):
        span = 2**bit
        node = seq // span
        columns = pl.ds(bit * head_dim, head_dim)

        @pl.when(lax.rem(node, 2) == 1)
        def _():
            total = jnp.zeros((head_dim, head_dim), F32)
            for offset in range(span):
                total += states_ref[(node - 1) * span + offset].astype(F32)
            upper = total.astype(BF16)
            flat_ref[pl.ds(0, head_dim), columns] = upper
            flat_ref[pl.ds(head_dim, head_dim), columns] = (total - upper.astype(F32)).astype(BF16)

        @pl.when(lax.rem(node, 2) == 0)
        def _():
            flat_ref[:, columns] = jnp.zeros((2 * head_dim, head_dim), BF16)

    def ring_copy(way, origin, c):
        return pltpu.make_async_remote_copy(
            src_ref=gather_ref.at[origin, c], dst_ref=gather_ref.at[origin, c],
            send_sem=ring_send.at[way], recv_sem=ring_recv.at[origin, c],
            device_id=(seq, neighbours[way]), device_id_type=MESH,
        )

    def passes(way, c):
        place = places[way]
        return jnp.logical_or(place + 1 < last, jnp.logical_and(place < last, kept(way, c)))

    def relay(way, distance, i):
        origin = origin_of(way, distance)
        c = tile_of(origin, i)
        ring_copy(way, origin, c).wait_recv()

        @pl.when(passes(way, c))
        def _():
            ring_copy(way, origin, c).start()

    def attn_tile(i):
        rows = pl.ds(pl.multiple_of(i * TILE, TILE), TILE)
        query = q_ref[rows, :]
        readout = dot(jnp.concatenate([query, query], axis=1), flat_ref[...], 1, 0)
        coeff = coeff_ref[rows, :]
        cross = jnp.zeros((TILE, head_dim), F32)
        for bit in range(seq_bits):
            level = local_bits + 1 + bit
            cross += coeff[:, level : level + 1] * readout[:, bit * head_dim : (bit + 1) * head_dim]
        total = total_ref[rows, :] + cross
        normed = total * lax.rsqrt(jnp.mean(total * total, axis=1, keepdims=True) + EPSILON)
        attn_ref[rows, :] = normed.astype(BF16)
        gather_ref[head, i] = normed.T.astype(BF16)

    def middle(way):
        return jnp.logical_and(places[way] >= 2, places[way] < last)

    early_tiles = BURST * spare

    def produce(local):
        def step(t, carry):
            tile = tile_of(head, t)
            attn_tile(tile)
            if local:
                local_tile(tile_of(head, t + ahead))
            for way in range(2):
                @pl.when(passes(way, tile))
                def _():
                    ring_copy(way, head, tile).start()
            if not local:
                for way in range(2):
                    @pl.when(jnp.logical_and(middle(way), t >= keep))
                    def _():
                        for i in range(BURST):
                            relay(way, 1, BURST * (t - keep) + i)
            return carry
        return step

    with jax.named_scope("phase1a"):
        lax.fori_loop(0, tiles - ahead, produce(True), 0)
    with jax.named_scope("phase1b"):
        lax.fori_loop(tiles - ahead, tiles, produce(False), 0)

    def joined(origin, q):
        return jnp.concatenate([gather_ref[origin, 4 * q + i] for i in range(4)], axis=1)

    def multiply(origin, q):
        rows = pl.ds(pl.multiple_of(q * (4 * TILE), 4 * TILE), 4 * TILE)
        acc_ref[origin] += dot(joined(origin, q), cot_ref[rows, :], 1, 0)

    def multiply_help(way, origin, i):
        rows = pl.ds(pl.multiple_of(i * (4 * TILE), 4 * TILE), 4 * TILE)
        acc_ref[n_head + origin] += dot(joined(origin, i if way == 0 else keep // 4 + i), help_ref[rows, :], 1, 0)

    def share_copy(slot, target):
        return pltpu.make_async_remote_copy(
            src_ref=share_ref.at[slot, pl.ds(target * rows_per, rows_per), :],
            dst_ref=shares_ref.at[slot, lax.rem(seq - target + n_seq, n_seq) - 1],
            send_sem=share_send.at[slot], recv_sem=share_recv.at[slot],
            device_id=(target, head), device_id_type=MESH,
        )

    def send_share(slot):
        share_ref[slot] = (acc_ref[slot] * scale).astype(BF16)
        for target in range(reducers):
            @pl.when(seq != target)
            def _():
                share_copy(slot, target).start()

    def final_copy(slot, block, origin, kind, owner):
        columns = pl.ds(owner * piece if piece < width else 0, piece)
        return pltpu.make_async_remote_copy(
            src_ref=final_ref.at[slot, :, columns] if piece < width else final_ref.at[slot],
            dst_ref=finals_ref.at[kind, pl.ds(pl.multiple_of(seq * rows_per, rows_per), rows_per), :],
            send_sem=final_send.at[slot], recv_sem=final_recv.at[kind],
            device_id=(block * owners + owner, origin), device_id_type=MESH,
        )

    def is_self(block, origin, owner):
        return jnp.logical_and(block * owners + owner == seq, origin == head)

    def reduce_share(slot, block, origin, kind):
        @pl.when(seq < reducers)
        def _():
            mine = pl.ds(pl.multiple_of(seq * rows_per, rows_per), rows_per)
            arrived = shares_ref.at[slot]
            pltpu.make_async_remote_copy(
                src_ref=arrived, dst_ref=arrived,
                send_sem=share_send.at[slot], recv_sem=share_recv.at[slot],
                device_id=(0, head), device_id_type=MESH,
            ).wait_recv()
            whole = acc_ref[slot, mine, :] * scale
            for source in range(n_seq - 1):
                whole += shares_ref[slot, source].astype(F32)
            final_ref[slot] = whole
            for owner in range(owners):
                @pl.when(jnp.logical_not(is_self(block, origin, owner)))
                def _():
                    final_copy(slot, block, origin, kind, owner).start()

                @pl.when(is_self(block, origin, owner))
                def _():
                    start = owner * piece if piece < width else 0
                    finals_ref[kind, mine, :] = final_ref[slot, :, pl.ds(start, piece)]

    loads[5].wait()

    def arrive(way, origin, q):
        for c in range(4):
            ring_copy(way, origin, 4 * q + c).wait_recv()

    def helper(way):
        return jnp.logical_and(places[way] == last - 1, helps)

    def block_of(way):
        return last if way == 0 else 0

    def every_group(distance, act):
        @pl.when(distance == 0)
        def _():
            act(head, head, head, 0)
            if helps:
                for way in range(2):
                    pl.when(helper(way))(functools.partial(act, n_head + head, block_of(way), head, 1))

        for way in range(2):
            origin = origin_of(way, distance)

            @pl.when(jnp.logical_and(distance > 0, distance < places[way]))
            def _():
                act(origin, head, origin, 0)
                if helps:
                    pl.when(helper(way))(functools.partial(act, n_head + origin, block_of(way), origin, 1))

    began = early_tiles
    if last > 3:
        began = tiles
        for way in range(2):
            def rest(i, carry):
                relay(way, 1, i)
                return carry

            def more(n, carry):
                relay(way, 2 + n // tiles, lax.rem(n, tiles))
                return carry

            @pl.when(middle(way))
            def _():
                lax.fori_loop(early_tiles, tiles, rest, 0)
                lax.fori_loop(0, (places[way] - 2) * tiles, more, 0)

    farthest = jnp.maximum(places[0], places[1])

    def flow(u, carry):
        for way in range(2):
            place, origin = places[way], block_of(1 - way)
            i = u - 1 - LAG * (place - 1)

            if began < tiles:
                @pl.when(jnp.logical_and(middle(way), u < tiles - began))
                def _():
                    relay(way, 1, began + u)

            @pl.when(jnp.logical_and(jnp.logical_and(place > 0, place < last), jnp.logical_and(i >= 0, i < tiles)))
            def _():
                relay(way, place, i)

        for way in range(2):
            place, origin = places[way], block_of(1 - way)
            i = u - 1 - LAG * (place - 1)
            j = i // 4
            q = quad_of(origin, j)

            @pl.when(jnp.logical_and(jnp.logical_and(place > 0, i - 4 * j == 3), jnp.logical_and(i >= 0, i < tiles)))
            def _():
                @pl.when(jnp.logical_or(place < last, kept_quad(way, q)))
                def _():
                    pl.when(place == last)(functools.partial(arrive, way, origin, q))
                    multiply(origin, q)
                if helps:
                    @pl.when(jnp.logical_and(helper(way), jnp.logical_not(kept_quad(way, q))))
                    def _():
                        multiply_help(way, origin, 0)
                        send_share(n_head + origin)
                pl.when(j == quads - 1)(functools.partial(send_share, origin))

        distance = u // quads
        j = u - quads * distance

        @pl.when(distance == 0)
        def _():
            multiply(head, quad_of(head, j))

        for way in range(2):
            place, origin = places[way], origin_of(way, distance)
            q = quad_of(origin, j)

            @pl.when(jnp.logical_and(jnp.logical_and(distance > 0, distance < place), jnp.logical_or(place < last, kept_quad(way, q))))
            def _():
                pl.when(place == last)(functools.partial(arrive, way, origin, q))
                multiply(origin, q)

            if helps:
                @pl.when(jnp.logical_and(helper(way), jnp.logical_and(distance < place, j == quads - 1)))
                def _():
                    @pl.when(distance == 0)
                    def _():
                        for i in range(spare):
                            help_copy(way, i).wait_recv()
                    multiply_help(way, origin, 0)

        @pl.when(j == quads - 1)
        def _():
            every_group(distance, lambda slot, *_: send_share(slot))
            pl.when(jnp.logical_and(farthest == last, distance >= 2))(lambda: every_group(distance - 2, reduce_share))
        return carry

    with jax.named_scope("flow"):
        lax.fori_loop(0, jnp.maximum(tiles + 1 + LAG * (farthest - 1), quads * (farthest + 2)), flow, 0)

    ends = []
    for way in range(2):
        place, origin = places[way], block_of(1 - way)
        if helps:
            ends.append((helper(way), n_head + origin, block_of(way), origin, 1))
    for way in range(2):
        place, origin = places[way], block_of(1 - way)
        ends.append((place > 0, origin, head, origin, 0))
    with jax.named_scope("reducelast"):
        @pl.when(farthest < last)
        def _():
            def one(distance, carry):
                every_group(distance, reduce_share)
                return carry

            lax.fori_loop(0, farthest, one, 0)

        for condition, *rest in ends[:-2]:
            pl.when(condition)(functools.partial(reduce_share, *rest))
        closer = places[0] <= places[1]
        for flip, pair in ((closer, ends[-2:]), (jnp.logical_not(closer), ends[-2:][::-1])):
            @pl.when(flip)
            def _():
                for condition, *rest in pair:
                    pl.when(condition)(functools.partial(reduce_share, *rest))

    with jax.named_scope("finals"):
        home = seq // owners
        at_end = jnp.logical_and(jnp.logical_or(home == 0, home == last), head != home)
        for kind in range(2 if helps else 1):
            plane = home if kind == 0 else jnp.where(home == 0, 1, last - 1)
            own = jnp.logical_and(seq < reducers, head == plane)
            expected = at_end if kind else seq >= 0
            for count, match in ((reducers - 1, own), (reducers, jnp.logical_not(own))):
                @pl.when(jnp.logical_and(expected, match))
                def _():
                    arrived = finals_ref.at[kind, pl.ds(0, count * rows_per), :]
                    pltpu.make_async_remote_copy(
                        src_ref=arrived, dst_ref=arrived,
                        send_sem=final_send.at[0], recv_sem=final_recv.at[kind],
                        device_id=(0, plane), device_id_type=MESH,
                    ).wait_recv()
        if helps:
            @pl.when(at_end)
            def _():
                finals_ref[0] += finals_ref[1]
        per = grad_ref.shape[1]
        if per == piece:
            grad_ref[...] = finals_ref[0]
        else:
            for owner in range(owners):
                @pl.when(lax.rem(seq, owners) == owner)
                def _():
                    grad_ref[...] = finals_ref[0][:, owner * per : (owner + 1) * per]

    with jax.named_scope("drain"):
        for block in range(n_seq - 1):
            @pl.when(seq == block)
            def _():
                sent = states_ref.at[pl.ds(0, n_seq - 1 - block)]
                pltpu.make_async_remote_copy(
                    src_ref=sent, dst_ref=sent,
                    send_sem=state_send.at[0], recv_sem=state_recv.at[0],
                    device_id=(0, head), device_id_type=MESH,
                ).wait_send()
        for way in range(2):
            if helps:
                @pl.when(places[way] == last)
                def _():
                    pltpu.make_async_remote_copy(
                        src_ref=help_ref, dst_ref=help_ref,
                        send_sem=help_send.at[0], recv_sem=help_recv.at[0],
                        device_id=(seq, left if way == 0 else right), device_id_type=MESH,
                    ).wait_send()
            for place in range(last):
                @pl.when(places[way] == place)
                def _():
                    count = tiles if place + 1 < last else keep
                    sent = gather_ref.at[pl.ds(0, place + 1), pl.ds(0, count)]
                    pltpu.make_async_remote_copy(
                        src_ref=sent, dst_ref=sent,
                        send_sem=ring_send.at[way], recv_sem=ring_recv.at[0, 0],
                        device_id=(seq, neighbours[way]), device_id_type=MESH,
                    ).wait_send()
        def drain(slot, block, origin, kind):
            def sent_shares(count):
                sent = share_ref.at[slot, pl.ds(0, count * rows_per), :]
                pltpu.make_async_remote_copy(
                    src_ref=sent, dst_ref=sent,
                    send_sem=share_send.at[slot], recv_sem=share_recv.at[slot],
                    device_id=(0, head), device_id_type=MESH,
                ).wait_send()

            def sent_finals(count):
                sent = finals_ref.at[0, pl.ds(0, count * rows_per), :]
                pltpu.make_async_remote_copy(
                    src_ref=sent, dst_ref=sent,
                    send_sem=final_send.at[slot], recv_sem=final_recv.at[0],
                    device_id=(0, head), device_id_type=MESH,
                ).wait_send()

            pl.when(seq < reducers)(lambda: sent_shares(reducers - 1))
            if reducers < n_seq:
                pl.when(seq >= reducers)(lambda: sent_shares(reducers))
            near = jnp.logical_and(seq // owners == block, origin == head)
            pl.when(jnp.logical_and(seq < reducers, jnp.logical_not(near)))(lambda: sent_finals(owners))
            if owners > 1:
                pl.when(jnp.logical_and(seq < reducers, near))(lambda: sent_finals(owners - 1))

        for origin in range(n_head):
            drain(origin, head, origin, 0)
        if helps:
            for way in range(2):
                for origin in range(n_head):
                    @pl.when(jnp.logical_and(helper(way), origin != block_of(way)))
                    def _():
                        drain(n_head + origin, block_of(way), origin, 1)


def finish(attn_ref, grad_ref, attn_out, grad_out, turned_ref, sem):
    attn_copy = pltpu.make_async_copy(attn_ref, attn_out, sem.at[0])
    attn_copy.start()
    turned_ref[...] = grad_ref[...].T
    grad_copy = pltpu.make_async_copy(turned_ref, grad_out, sem.at[1])
    grad_copy.start()
    attn_copy.wait()
    grad_copy.wait()


def body(n_seq, n_head, queries, keys, values, level_ids, level_table, out_cotangent):
    block_len, head_dim = queries.shape
    width = out_cotangent.shape[1]
    per = width * n_head // n_seq
    piece = per if per % 128 == 0 else width
    seq_bits = n_seq.bit_length() - 1
    tiles = block_len // TILE
    inner = tiles.bit_length() - 1
    rows_per = max(16, head_dim // n_seq)
    slots = 2 * n_head
    spare = max(4, tiles - kept_tiles(n_head, tiles))
    dma = pltpu.SemaphoreType.DMA
    vmem = pl.BlockSpec(memory_space=pltpu.VMEM)
    hbm = pl.BlockSpec(memory_space=pltpu.HBM)
    attn_out, grad = pl.pallas_call(
        functools.partial(kernel, n_seq, n_head),
        out_shape=(
            pltpu.VMEM((block_len, head_dim), BF16),
            pltpu.VMEM((head_dim, per), F32),
        ),
        in_specs=[hbm] * 6,
        out_specs=(vmem, vmem),
        scratch_shapes=[
            pltpu.VMEM((block_len, head_dim), BF16),
            pltpu.VMEM((block_len, head_dim), BF16),
            pltpu.VMEM((block_len, head_dim), BF16),
            pltpu.VMEM((block_len, width), BF16),
            pltpu.VMEM((1, block_len), jnp.int32),
            pltpu.VMEM(level_table.shape[::-1], F32),
            pltpu.VMEM((TILE, TILE), jnp.int32),
            pltpu.VMEM((block_len, level_table.shape[1]), F32),
            pltpu.VMEM((block_len, head_dim), F32),
            pltpu.VMEM((tiles, head_dim, inner * head_dim), BF16),
            pltpu.VMEM((head_dim, head_dim), BF16),
            pltpu.VMEM((n_seq, head_dim, head_dim), BF16),
            pltpu.VMEM((2 * head_dim, seq_bits * head_dim), BF16),
            pltpu.VMEM((n_head, tiles, head_dim, TILE), BF16),
            pltpu.VMEM((slots, head_dim, width), F32),
            pltpu.VMEM((slots, head_dim, width), BF16),
            pltpu.VMEM((slots, n_seq - 1, rows_per, width), BF16),
            pltpu.VMEM((slots, rows_per, width), F32),
            pltpu.VMEM((2, head_dim, piece), F32),
            pltpu.VMEM((spare * TILE, width), BF16),
            dma((6,)),
            dma((1,)),
            dma((1,)),
            dma((2,)),
            dma((n_head, tiles)),
            dma((slots,)),
            dma((slots,)),
            dma((slots,)),
            dma((2,)),
            dma((1,)),
            dma((spare,)),
        ],
        compiler_params=pltpu.CompilerParams(
            collective_id=0, has_side_effects=True, vmem_limit_bytes=60 * 2**20
        ),
    )(queries, keys, values, level_ids[None, :], level_table.T, out_cotangent)
    return pl.pallas_call(
        finish,
        out_shape=(
            jax.ShapeDtypeStruct((block_len, head_dim), BF16),
            jax.ShapeDtypeStruct((per, head_dim), F32),
        ),
        in_specs=[vmem, vmem],
        out_specs=(hbm, hbm),
        scratch_shapes=[pltpu.VMEM((per, head_dim), F32), dma((2,))],
        compiler_params=pltpu.CompilerParams(vmem_limit_bytes=4 * 2**20),
    )(attn_out, grad)


def solution(mesh):
    in_specs = (
        P("seq", "head"),
        P("seq", "head"),
        P("seq", "head"),
        P("seq"),
        P(),
        P("seq", "head"),
    )
    out_specs = (P("seq", "head"), P("seq", "head"))
    return jax.shard_map(
        functools.partial(body, mesh.shape["seq"], mesh.shape["head"]),
        mesh=mesh, in_specs=in_specs, out_specs=out_specs, check_vma=False,
    )
```

```python
import functools

import jax
import jax.numpy as jnp
from jax import lax
from jax.experimental import pallas as pl
from jax.experimental.pallas import tpu as pltpu
from jax.sharding import PartitionSpec as P

EPSILON = 1e-06
TILE = 128
KEEP = 12
AHEAD = 8
LEAD = 4
LAG = 6
BURST = 2
MESH = pl.DeviceIdType.MESH
F32 = jnp.float32
BF16 = jnp.bfloat16


def dot(a, b, ca, cb):
    return lax.dot_general(a, b, (((ca,), (cb,)), ((), ())), preferred_element_type=F32)


def tile_levels(tile):
    row = lax.broadcasted_iota(jnp.int32, (tile, tile), 0)
    col = lax.broadcasted_iota(jnp.int32, (tile, tile), 1)
    apart = jnp.bitwise_xor(row, col)
    levels = jnp.zeros((tile, tile), jnp.int32)
    for bit in range(tile.bit_length() - 1):
        levels = levels + (jnp.right_shift(apart, bit) > 0).astype(jnp.int32)
    return jnp.where(col <= row, levels, -1)


def kept_tiles(n_head, tiles):
    return tiles * KEEP // 16 if n_head >= 4 else tiles


def kernel(
    n_seq, n_head,
    q_hbm, k_hbm, v_hbm, ids_hbm, table_hbm, cot_hbm,
    attn_ref, grad_ref,
    q_ref, k_ref, v_ref, cot_ref, ids_ref, table_ref, levels_ref, coeff_ref, total_ref, sib_ref,
    state_ref, states_ref, flat_ref, gather_ref, acc_ref,
    share_ref, shares_ref, final_ref, finals_ref, help_ref,
    load_sem, state_send, state_recv, ring_send, ring_recv,
    share_send, share_recv, final_send, final_recv, help_send, help_recv,
):
    seq, head = lax.axis_index("seq"), lax.axis_index("head")
    block_len, head_dim = q_ref.shape
    width = cot_ref.shape[1]
    tiles = block_len // TILE
    pairs = tiles // 2
    tile_bits = TILE.bit_length() - 1
    local_bits = block_len.bit_length() - 1
    inner = local_bits - tile_bits
    seq_bits = n_seq.bit_length() - 1
    owners = n_seq // n_head
    rows_per = max(16, head_dim // n_seq)
    reducers = head_dim // rows_per
    piece = finals_ref.shape[2]
    last = n_head - 1
    keep = kept_tiles(n_head, tiles)
    helps = keep < tiles
    quads = tiles // 4
    ahead = min(AHEAD, tiles)
    lead = min(LEAD, ahead)
    scale = (block_len * n_seq) ** (-0.5)

    loads = [
        pltpu.make_async_copy(src, dst, load_sem.at[i])
        for i, (src, dst) in enumerate(
            [
                (k_hbm, k_ref), (v_hbm, v_ref), (table_hbm, table_ref), (ids_hbm, ids_ref),
                (q_hbm, q_ref), (cot_hbm, cot_ref),
            ]
        )
    ]
    for load in loads[:4]:
        load.start()

    barrier = pltpu.get_barrier_semaphore()

    def greet(device):
        pl.semaphore_signal(barrier, inc=1, device_id=device, device_id_type=MESH)

    for step in range(1, n_seq):
        greet((lax.rem(seq + step, n_seq), head))
    pl.when(head > 0)(lambda: greet((seq, head - 1)))
    pl.when(head < n_head - 1)(lambda: greet((seq, head + 1)))

    levels_ref[...] = tile_levels(TILE)
    with jax.named_scope("kv"):
        for load in loads[:4]:
            load.wait()
    for load in loads[4:]:
        load.start()
    table = table_ref[...]
    high = table.astype(BF16)
    rest = table - high.astype(F32)
    mid = rest.astype(BF16)
    low = (rest - mid.astype(F32)).astype(BF16)
    table3 = jnp.concatenate([high, mid, low], axis=1)

    nodes = [
        dot(k_ref[pl.ds(i * TILE, TILE), :], v_ref[pl.ds(i * TILE, TILE), :], 0, 0)
        for i in range(tiles)
    ]
    for bit in range(inner):
        for i in range(tiles):
            place = (i >> bit) ^ 1
            value = nodes[place].astype(BF16) if (i >> bit) & 1 else jnp.zeros((head_dim, head_dim), BF16)
            sib_ref[i, :, pl.ds(bit * head_dim, head_dim)] = value
        nodes = [nodes[2 * i] + nodes[2 * i + 1] for i in range(len(nodes) // 2)]
    state_ref[...] = nodes[0].astype(BF16)


    def local_tile(i):
        rows = pl.ds(pl.multiple_of(i * TILE, TILE), TILE)
        row_ids = lax.broadcasted_iota(jnp.int32, (table.shape[1], TILE), 0)
        onehot = (row_ids == ids_ref[:, rows]).astype(F32).astype(BF16)
        coeff = dot(jnp.concatenate([onehot] * 3, axis=0), table3, 0, 1)
        coeff_ref[rows, :] = coeff
        levels = levels_ref[...]
        weights = jnp.zeros((TILE, TILE), F32)
        for level in range(tile_bits + 1):
            weights = jnp.where(levels == level, coeff[:, level : level + 1], weights)
        query = q_ref[rows, :]
        scores = dot(query, k_ref[rows, :], 1, 1)
        total = dot((weights * scores).astype(BF16), v_ref[rows, :], 1, 0)
        readout = dot(query, sib_ref[i], 1, 0)
        for bit in range(inner):
            level = tile_bits + 1 + bit
            total += coeff[:, level : level + 1] * readout[:, bit * head_dim : (bit + 1) * head_dim]
        total_ref[rows, :] = total

    def local_tiles(start, stop):
        def one(i, carry):
            local_tile(tile_of(head, i))
            return carry

        lax.fori_loop(start, stop, one, 0, unroll=True)

    with jax.named_scope("barrier"):
        pl.semaphore_wait(barrier, n_seq - 1 + jnp.minimum(head, 1) + jnp.minimum(last - head, 1))

    def state_copy(target):
        return pltpu.make_async_remote_copy(
            src_ref=state_ref, dst_ref=states_ref.at[seq],
            send_sem=state_send.at[0], recv_sem=state_recv.at[0],
            device_id=(target, head), device_id_type=MESH,
        )

    def partner(k):
        place = 0
        for bit in range(seq_bits):
            mine = lax.rem(seq // 2**bit, 2)
            place += 2**bit * (1 - mine if (k >> bit) & 1 else mine)
        return place

    for k in range(n_seq - 1, 0, -1):
        @pl.when(seq < partner(k))
        def _():
            state_copy(partner(k)).start()

    right, left = lax.rem(head + 1, n_head), lax.rem(head + n_head - 1, n_head)
    neighbours = (right, left)
    places = (head, last - head)

    half = n_head // 2
    spare = tiles - keep

    def origin_of(way, distance):
        return head - distance if way == 0 else head + distance

    def upward(origin):
        inside = jnp.logical_and(origin > 0, origin < half)
        return jnp.logical_or(inside, origin == last)

    def tile_of(origin, i):
        return jnp.where(upward(origin), i, tiles - 1 - i)

    def quad_of(origin, j):
        return jnp.where(upward(origin), j, quads - 1 - j)

    def kept(way, c):
        return c >= spare if way == 0 else c < keep

    def kept_quad(way, q):
        return 4 * q >= spare if way == 0 else 4 * q < keep

    def help_copy(way, i):
        return pltpu.make_async_remote_copy(
            src_ref=cot_hbm.at[pl.ds(i * TILE if way == 0 else (keep + i) * TILE, TILE), :],
            dst_ref=help_ref.at[pl.ds(i * TILE, TILE), :],
            send_sem=help_send.at[0], recv_sem=help_recv.at[0],
            device_id=(seq, left if way == 0 else right), device_id_type=MESH,
        )

    for way in range(2):
        @pl.when(places[way] == last)
        def _():
            for i in range(spare):
                help_copy(way, i).start()

    loads[4].wait()
    with jax.named_scope("local1"):
        local_tiles(0, ahead)
    acc_ref[...] = jnp.zeros_like(acc_ref)

    with jax.named_scope("states"):
        for block in range(1, n_seq):
            @pl.when(seq == block)
            def _():
                arrived = states_ref.at[pl.ds(0, block)]
                pltpu.make_async_remote_copy(
                    src_ref=arrived, dst_ref=arrived,
                    send_sem=state_send.at[0], recv_sem=state_recv.at[0],
                    device_id=(0, head), device_id_type=MESH,
                ).wait_recv()

    for bit in range(seq_bits):
        span = 2**bit
        node = seq // span
        columns = pl.ds(bit * head_dim, head_dim)

        @pl.when(lax.rem(node, 2) == 1)
        def _():
            total = jnp.zeros((head_dim, head_dim), F32)
            for offset in range(span):
                total += states_ref[(node - 1) * span + offset].astype(F32)
            upper = total.astype(BF16)
            flat_ref[pl.ds(0, head_dim), columns] = upper
            flat_ref[pl.ds(head_dim, head_dim), columns] = (total - upper.astype(F32)).astype(BF16)

        @pl.when(lax.rem(node, 2) == 0)
        def _():
            flat_ref[:, columns] = jnp.zeros((2 * head_dim, head_dim), BF16)

    def ring_copy(way, origin, c):
        return pltpu.make_async_remote_copy(
            src_ref=gather_ref.at[origin, c], dst_ref=gather_ref.at[origin, c],
            send_sem=ring_send.at[way], recv_sem=ring_recv.at[origin - way, c],
            device_id=(seq, neighbours[way]), device_id_type=MESH,
        )

    def passes(way, c):
        place = places[way]
        return jnp.logical_or(place + 1 < last, jnp.logical_and(place < last, kept(way, c)))

    def relay(way, distance, i):
        origin = origin_of(way, distance)
        c = tile_of(origin, i)
        ring_copy(way, origin, c).wait_recv()

        @pl.when(passes(way, c))
        def _():
            ring_copy(way, origin, c).start()

    def attn_tile(i):
        rows = pl.ds(pl.multiple_of(i * TILE, TILE), TILE)
        query = q_ref[rows, :]
        readout = dot(jnp.concatenate([query, query], axis=1), flat_ref[...], 1, 0)
        coeff = coeff_ref[rows, :]
        cross = jnp.zeros((TILE, head_dim), F32)
        for bit in range(seq_bits):
            level = local_bits + 1 + bit
            cross += coeff[:, level : level + 1] * readout[:, bit * head_dim : (bit + 1) * head_dim]
        total = total_ref[rows, :] + cross
        normed = total * lax.rsqrt(jnp.mean(total * total, axis=1, keepdims=True) + EPSILON)
        attn_ref[rows, :] = normed.astype(BF16)
        gather_ref[head, i] = normed.T.astype(BF16)

    def middle(way):
        return jnp.logical_and(places[way] >= 2, places[way] < last)

    early_tiles = BURST * spare

    def produce(local, relaying):
        def step(t, carry):
            tile = tile_of(head, t)
            attn_tile(tile)
            if local:
                local_tile(tile_of(head, t + ahead - lead))
            for way in range(2):
                @pl.when(passes(way, tile))
                def _():
                    ring_copy(way, head, tile).start()
            if relaying:
                for way in range(2):
                    @pl.when(jnp.logical_and(middle(way), t >= keep))
                    def _():
                        for i in range(BURST):
                            relay(way, 1, BURST * (t - keep) + i)
            return carry
        return step

    with jax.named_scope("phase1o"):
        lax.fori_loop(0, lead, produce(False, False), 0)
    with jax.named_scope("phase1a"):
        lax.fori_loop(lead, tiles - ahead + lead, produce(True, False), 0)
    with jax.named_scope("phase1b"):
        lax.fori_loop(tiles - ahead + lead, tiles, produce(False, True), 0)

    def joined(origin, q):
        return jnp.concatenate([gather_ref[origin, 4 * q + i] for i in range(4)], axis=1)

    def multiply(origin, q):
        rows = pl.ds(pl.multiple_of(q * (4 * TILE), 4 * TILE), 4 * TILE)
        acc_ref[origin] += dot(joined(origin, q), cot_ref[rows, :], 1, 0)

    def multiply_help(way, origin, i):
        rows = pl.ds(pl.multiple_of(i * (4 * TILE), 4 * TILE), 4 * TILE)
        acc_ref[n_head + origin] += dot(joined(origin, i if way == 0 else keep // 4 + i), help_ref[rows, :], 1, 0)

    def share_copy(slot, k):
        target = partner(k)
        return pltpu.make_async_remote_copy(
            src_ref=share_ref.at[slot, pl.ds(pl.multiple_of(target * rows_per, rows_per), rows_per), :],
            dst_ref=shares_ref.at[slot, k - 1],
            send_sem=share_send.at[slot], recv_sem=share_recv.at[slot],
            device_id=(target, head), device_id_type=MESH,
        )

    def send_share(slot):
        share_ref[slot] = (acc_ref[slot] * scale).astype(BF16)
        for k in range(n_seq - 1, 0, -1):
            if reducers == n_seq:
                share_copy(slot, k).start()
            else:
                pl.when(partner(k) < reducers)(lambda: share_copy(slot, k).start())

    def final_copy(slot, block, origin, kind, owner):
        columns = pl.ds(owner * piece if piece < width else 0, piece)
        return pltpu.make_async_remote_copy(
            src_ref=final_ref.at[slot, :, columns] if piece < width else final_ref.at[slot],
            dst_ref=finals_ref.at[kind, pl.ds(pl.multiple_of(seq * rows_per, rows_per), rows_per), :],
            send_sem=final_send.at[slot], recv_sem=final_recv.at[kind],
            device_id=(block * owners + owner, origin), device_id_type=MESH,
        )

    def is_self(block, origin, owner):
        return jnp.logical_and(block * owners + owner == seq, origin == head)

    def reduce_share(slot, block, origin, kind):
        @pl.when(seq < reducers)
        def _():
            mine = pl.ds(pl.multiple_of(seq * rows_per, rows_per), rows_per)
            arrived = shares_ref.at[slot]
            pltpu.make_async_remote_copy(
                src_ref=arrived, dst_ref=arrived,
                send_sem=share_send.at[slot], recv_sem=share_recv.at[slot],
                device_id=(0, head), device_id_type=MESH,
            ).wait_recv()
            whole = acc_ref[slot, mine, :] * scale
            for source in range(n_seq - 1):
                whole += shares_ref[slot, source].astype(F32)
            final_ref[slot] = whole
            for owner in range(owners):
                @pl.when(jnp.logical_not(is_self(block, origin, owner)))
                def _():
                    final_copy(slot, block, origin, kind, owner).start()

                @pl.when(is_self(block, origin, owner))
                def _():
                    start = owner * piece if piece < width else 0
                    finals_ref[kind, mine, :] = final_ref[slot, :, pl.ds(start, piece)]

    loads[5].wait()

    def arrive(way, origin, q):
        for c in range(4):
            ring_copy(way, origin, 4 * q + c).wait_recv()

    def helper(way):
        return jnp.logical_and(places[way] == last - 1, helps)

    def block_of(way):
        return last if way == 0 else 0

    def every_group(distance, act):
        @pl.when(distance == 0)
        def _():
            act(head, head, head, 0)
            if helps:
                for way in range(2):
                    pl.when(helper(way))(functools.partial(act, n_head + head, block_of(way), head, 1))

        for way in range(2):
            origin = origin_of(way, distance)

            @pl.when(jnp.logical_and(distance > 0, distance < places[way]))
            def _():
                act(origin, head, origin, 0)
                if helps:
                    pl.when(helper(way))(functools.partial(act, n_head + origin, block_of(way), origin, 1))

    began = early_tiles
    if last > 3:
        began = tiles
        for way in range(2):
            def rest(i, carry):
                relay(way, 1, i)
                return carry

            def more(n, carry):
                relay(way, 2 + n // tiles, lax.rem(n, tiles))
                return carry

            @pl.when(middle(way))
            def _():
                lax.fori_loop(early_tiles, tiles, rest, 0)
                lax.fori_loop(0, (places[way] - 2) * tiles, more, 0)

    farthest = jnp.maximum(places[0], places[1])

    def flow(u, carry):
        for way in range(2):
            place, origin = places[way], block_of(1 - way)
            i = u - 1 - LAG * (place - 1)

            if began < tiles:
                @pl.when(jnp.logical_and(middle(way), u < tiles - began))
                def _():
                    relay(way, 1, began + u)

            @pl.when(jnp.logical_and(jnp.logical_and(place > 0, place < last), jnp.logical_and(i >= 0, i < tiles)))
            def _():
                relay(way, place, i)

        for way in range(2):
            place, origin = places[way], block_of(1 - way)
            i = u - 1 - LAG * (place - 1)
            j = i // 4
            q = quad_of(origin, j)

            @pl.when(jnp.logical_and(jnp.logical_and(place > 0, i - 4 * j == 3), jnp.logical_and(i >= 0, i < tiles)))
            def _():
                @pl.when(jnp.logical_or(place < last, kept_quad(way, q)))
                def _():
                    pl.when(place == last)(functools.partial(arrive, way, origin, q))
                    multiply(origin, q)
                done = jnp.where(place == last, keep // 4 - 1, quads - 1)
                pl.when(j == done)(functools.partial(send_share, origin))
                if helps:
                    @pl.when(jnp.logical_and(helper(way), jnp.logical_not(kept_quad(way, q))))
                    def _():
                        multiply_help(way, origin, 0)
                        send_share(n_head + origin)

        distance = u // quads
        j = u - quads * distance

        @pl.when(distance == 0)
        def _():
            multiply(head, quad_of(head, j))

        for way in range(2):
            place, origin = places[way], origin_of(way, distance)
            q = quad_of(origin, j)

            @pl.when(jnp.logical_and(jnp.logical_and(distance > 0, distance < place), jnp.logical_or(place < last, kept_quad(way, q))))
            def _():
                pl.when(place == last)(functools.partial(arrive, way, origin, q))
                multiply(origin, q)

            if helps:
                @pl.when(jnp.logical_and(helper(way), jnp.logical_and(distance < place, j == quads - 1)))
                def _():
                    @pl.when(distance == 0)
                    def _():
                        pltpu.make_async_remote_copy(
                            src_ref=help_ref, dst_ref=help_ref,
                            send_sem=help_send.at[0], recv_sem=help_recv.at[0],
                            device_id=(seq, left if way == 0 else right), device_id_type=MESH,
                        ).wait_recv()
                    multiply_help(way, origin, 0)

        @pl.when(j == quads - 1)
        def _():
            every_group(distance, lambda slot, *_: send_share(slot))
            pl.when(jnp.logical_and(farthest == last, distance >= 2))(lambda: every_group(distance - 2, reduce_share))
        return carry

    with jax.named_scope("flow"):
        lax.fori_loop(0, jnp.maximum(tiles + 1 + LAG * (farthest - 1), quads * (farthest + 2)), flow, 0)

    ends = []
    for way in range(2):
        place, origin = places[way], block_of(1 - way)
        if helps:
            ends.append((helper(way), n_head + origin, block_of(way), origin, 1))
    for way in range(2):
        place, origin = places[way], block_of(1 - way)
        ends.append((place > 0, origin, head, origin, 0))
    with jax.named_scope("reducelast"):
        @pl.when(farthest < last)
        def _():
            def one(distance, carry):
                every_group(distance, reduce_share)
                return carry

            lax.fori_loop(0, farthest, one, 0)

        for condition, *rest in ends[:-2]:
            pl.when(condition)(functools.partial(reduce_share, *rest))
        closer = places[0] <= places[1]
        for flip, pair in ((closer, ends[-2:]), (jnp.logical_not(closer), ends[-2:][::-1])):
            @pl.when(flip)
            def _():
                for condition, *rest in pair:
                    pl.when(condition)(functools.partial(reduce_share, *rest))

    with jax.named_scope("finals"):
        home = seq // owners
        at_end = jnp.logical_and(jnp.logical_or(home == 0, home == last), head != home)
        for kind in range(2 if helps else 1):
            plane = home if kind == 0 else jnp.where(home == 0, 1, last - 1)
            own = jnp.logical_and(seq < reducers, head == plane)
            expected = at_end if kind else seq >= 0
            for count, match in ((reducers - 1, own), (reducers, jnp.logical_not(own))):
                @pl.when(jnp.logical_and(expected, match))
                def _():
                    arrived = finals_ref.at[kind, pl.ds(0, count * rows_per), :]
                    pltpu.make_async_remote_copy(
                        src_ref=arrived, dst_ref=arrived,
                        send_sem=final_send.at[0], recv_sem=final_recv.at[kind],
                        device_id=(0, plane), device_id_type=MESH,
                    ).wait_recv()
        if helps:
            @pl.when(at_end)
            def _():
                finals_ref[0] += finals_ref[1]
        per = grad_ref.shape[1]
        if per == piece:
            grad_ref[...] = finals_ref[0]
        else:
            for owner in range(owners):
                @pl.when(lax.rem(seq, owners) == owner)
                def _():
                    grad_ref[...] = finals_ref[0][:, owner * per : (owner + 1) * per]

    with jax.named_scope("drain"):
        for block in range(n_seq - 1):
            @pl.when(seq == block)
            def _():
                sent = states_ref.at[pl.ds(0, n_seq - 1 - block)]
                pltpu.make_async_remote_copy(
                    src_ref=sent, dst_ref=sent,
                    send_sem=state_send.at[0], recv_sem=state_recv.at[0],
                    device_id=(0, head), device_id_type=MESH,
                ).wait_send()
        for way in range(2):
            if helps:
                @pl.when(places[way] == last)
                def _():
                    pltpu.make_async_remote_copy(
                        src_ref=help_ref, dst_ref=help_ref,
                        send_sem=help_send.at[0], recv_sem=help_recv.at[0],
                        device_id=(seq, left if way == 0 else right), device_id_type=MESH,
                    ).wait_send()
            for place in range(last):
                @pl.when(places[way] == place)
                def _():
                    count = tiles if place + 1 < last else keep
                    sent = gather_ref.at[pl.ds(0, place + 1), pl.ds(0, count)]
                    pltpu.make_async_remote_copy(
                        src_ref=sent, dst_ref=sent,
                        send_sem=ring_send.at[way], recv_sem=ring_recv.at[0, 0],
                        device_id=(seq, neighbours[way]), device_id_type=MESH,
                    ).wait_send()
        def drain(slot, block, origin, kind):
            def sent_shares(count):
                sent = share_ref.at[slot, pl.ds(0, count * rows_per), :]
                pltpu.make_async_remote_copy(
                    src_ref=sent, dst_ref=sent,
                    send_sem=share_send.at[slot], recv_sem=share_recv.at[slot],
                    device_id=(0, head), device_id_type=MESH,
                ).wait_send()

            def sent_finals(count):
                sent = finals_ref.at[0, pl.ds(0, count * rows_per), :]
                pltpu.make_async_remote_copy(
                    src_ref=sent, dst_ref=sent,
                    send_sem=final_send.at[slot], recv_sem=final_recv.at[0],
                    device_id=(0, head), device_id_type=MESH,
                ).wait_send()

            pl.when(seq < reducers)(lambda: sent_shares(reducers - 1))
            if reducers < n_seq:
                pl.when(seq >= reducers)(lambda: sent_shares(reducers))
            near = jnp.logical_and(seq // owners == block, origin == head)
            pl.when(jnp.logical_and(seq < reducers, jnp.logical_not(near)))(lambda: sent_finals(owners))
            if owners > 1:
                pl.when(jnp.logical_and(seq < reducers, near))(lambda: sent_finals(owners - 1))

        for origin in range(n_head):
            drain(origin, head, origin, 0)
        if helps:
            for way in range(2):
                for origin in range(n_head):
                    @pl.when(jnp.logical_and(helper(way), origin != block_of(way)))
                    def _():
                        drain(n_head + origin, block_of(way), origin, 1)


def finish(attn_ref, grad_ref, attn_out, grad_out, turned_ref, sem):
    attn_copy = pltpu.make_async_copy(attn_ref, attn_out, sem.at[0])
    attn_copy.start()
    turned_ref[...] = grad_ref[...].T
    grad_copy = pltpu.make_async_copy(turned_ref, grad_out, sem.at[1])
    grad_copy.start()
    attn_copy.wait()
    grad_copy.wait()


def body(n_seq, n_head, queries, keys, values, level_ids, level_table, out_cotangent):
    block_len, head_dim = queries.shape
    width = out_cotangent.shape[1]
    per = width * n_head // n_seq
    piece = per if per % 128 == 0 else width
    seq_bits = n_seq.bit_length() - 1
    tiles = block_len // TILE
    inner = tiles.bit_length() - 1
    rows_per = max(16, head_dim // n_seq)
    slots = 2 * n_head
    spare = max(4, tiles - kept_tiles(n_head, tiles))
    dma = pltpu.SemaphoreType.DMA
    vmem = pl.BlockSpec(memory_space=pltpu.VMEM)
    hbm = pl.BlockSpec(memory_space=pltpu.HBM)
    attn_out, grad = pl.pallas_call(
        functools.partial(kernel, n_seq, n_head),
        out_shape=(
            pltpu.VMEM((block_len, head_dim), BF16),
            pltpu.VMEM((head_dim, per), F32),
        ),
        in_specs=[hbm] * 6,
        out_specs=(vmem, vmem),
        scratch_shapes=[
            pltpu.VMEM((block_len, head_dim), BF16),
            pltpu.VMEM((block_len, head_dim), BF16),
            pltpu.VMEM((block_len, head_dim), BF16),
            pltpu.VMEM((block_len, width), BF16),
            pltpu.VMEM((1, block_len), jnp.int32),
            pltpu.VMEM(level_table.shape[::-1], F32),
            pltpu.VMEM((TILE, TILE), jnp.int32),
            pltpu.VMEM((block_len, level_table.shape[1]), F32),
            pltpu.VMEM((block_len, head_dim), F32),
            pltpu.VMEM((tiles, head_dim, inner * head_dim), BF16),
            pltpu.VMEM((head_dim, head_dim), BF16),
            pltpu.VMEM((n_seq, head_dim, head_dim), BF16),
            pltpu.VMEM((2 * head_dim, seq_bits * head_dim), BF16),
            pltpu.VMEM((n_head, tiles, head_dim, TILE), BF16),
            pltpu.VMEM((slots, head_dim, width), F32),
            pltpu.VMEM((slots, head_dim, width), BF16),
            pltpu.VMEM((slots, n_seq - 1, rows_per, width), BF16),
            pltpu.VMEM((slots, rows_per, width), F32),
            pltpu.VMEM((2, head_dim, piece), F32),
            pltpu.VMEM((spare * TILE, width), BF16),
            dma((6,)),
            dma((1,)),
            dma((1,)),
            dma((2,)),
            dma((max(1, n_head - 1), tiles)),
            dma((slots,)),
            dma((slots,)),
            dma((slots,)),
            dma((2,)),
            dma((1,)),
            dma((1,)),
        ],
        compiler_params=pltpu.CompilerParams(
            collective_id=0, has_side_effects=True, vmem_limit_bytes=60 * 2**20
        ),
    )(queries, keys, values, level_ids[None, :], level_table.T, out_cotangent)
    return pl.pallas_call(
        finish,
        out_shape=(
            jax.ShapeDtypeStruct((block_len, head_dim), BF16),
            jax.ShapeDtypeStruct((per, head_dim), F32),
        ),
        in_specs=[vmem, vmem],
        out_specs=(hbm, hbm),
        scratch_shapes=[pltpu.VMEM((per, head_dim), F32), dma((2,))],
        compiler_params=pltpu.CompilerParams(vmem_limit_bytes=4 * 2**20),
    )(attn_out, grad)


def solution(mesh):
    in_specs = (
        P("seq", "head"),
        P("seq", "head"),
        P("seq", "head"),
        P("seq"),
        P(),
        P("seq", "head"),
    )
    out_specs = (P("seq", "head"), P("seq", "head"))
    return jax.shard_map(
        functools.partial(body, mesh.shape["seq"], mesh.shape["head"]),
        mesh=mesh, in_specs=in_specs, out_specs=out_specs, check_vma=False,
    )
```

```python
import functools

import jax
import jax.numpy as jnp
from jax import lax
from jax.experimental import pallas as pl
from jax.experimental.pallas import tpu as pltpu
from jax.sharding import PartitionSpec as P

EPSILON = 1e-06
TILE = 128
KEEP = 11
AHEAD = 8
LEAD = 6
LAG = 5
BURST = 2
MESH = pl.DeviceIdType.MESH
F32 = jnp.float32
BF16 = jnp.bfloat16


def dot(a, b, ca, cb):
    return lax.dot_general(a, b, (((ca,), (cb,)), ((), ())), preferred_element_type=F32)


def tile_levels(tile):
    row = lax.broadcasted_iota(jnp.int32, (tile, tile), 0)
    col = lax.broadcasted_iota(jnp.int32, (tile, tile), 1)
    apart = jnp.bitwise_xor(row, col)
    levels = jnp.zeros((tile, tile), jnp.int32)
    for bit in range(tile.bit_length() - 1):
        levels = levels + (jnp.right_shift(apart, bit) > 0).astype(jnp.int32)
    return jnp.where(col <= row, levels, -1)


def kept_tiles(n_head, tiles):
    return tiles * KEEP // 16 if n_head >= 4 else tiles


def kernel(
    n_seq, n_head,
    q_hbm, k_hbm, v_hbm, ids_hbm, table_hbm, cot_hbm,
    attn_ref, grad_ref,
    q_ref, k_ref, v_ref, cot_ref, ids_ref, table_ref, levels_ref, coeff_ref, total_ref, sib_ref,
    state_ref, states_ref, flat_ref, gather_ref, acc_ref,
    share_ref, shares_ref, final_ref, finals_ref, whole_ref, help_ref,
    load_sem, state_send, state_recv, ring_send, ring_recv,
    share_send, share_recv, final_send, final_recv, help_send, help_recv,
):
    seq, head = lax.axis_index("seq"), lax.axis_index("head")
    block_len, head_dim = q_ref.shape
    width = cot_ref.shape[1]
    tiles = block_len // TILE
    pairs = tiles // 2
    tile_bits = TILE.bit_length() - 1
    local_bits = block_len.bit_length() - 1
    inner = local_bits - tile_bits
    seq_bits = n_seq.bit_length() - 1
    owners = n_seq // n_head
    rows_per = max(16, head_dim // n_seq)
    reducers = head_dim // rows_per
    piece = finals_ref.shape[2]
    last = n_head - 1
    keep = kept_tiles(n_head, tiles)
    helps = keep < tiles
    quads = tiles // 4
    ahead = min(AHEAD, tiles)
    lead = min(LEAD, ahead)
    scale = (block_len * n_seq) ** (-0.5)

    loads = [
        pltpu.make_async_copy(src, dst, load_sem.at[i])
        for i, (src, dst) in enumerate(
            [
                (k_hbm, k_ref), (v_hbm, v_ref), (table_hbm, table_ref), (ids_hbm, ids_ref),
                (q_hbm, q_ref), (cot_hbm, cot_ref),
            ]
        )
    ]
    for load in loads[:4]:
        load.start()

    barrier = pltpu.get_barrier_semaphore()

    def greet(device):
        pl.semaphore_signal(barrier, inc=1, device_id=device, device_id_type=MESH)

    for step in range(1, n_seq):
        greet((lax.rem(seq + step, n_seq), head))
    pl.when(head > 0)(lambda: greet((seq, head - 1)))
    pl.when(head < n_head - 1)(lambda: greet((seq, head + 1)))

    levels_ref[...] = tile_levels(TILE)
    with jax.named_scope("kv"):
        for load in loads[:4]:
            load.wait()
    for load in loads[4:]:
        load.start()
    table = table_ref[...]
    high = table.astype(BF16)
    rest = table - high.astype(F32)
    mid = rest.astype(BF16)
    low = (rest - mid.astype(F32)).astype(BF16)
    table3 = jnp.concatenate([high, mid, low], axis=1)

    nodes = [
        dot(k_ref[pl.ds(i * TILE, TILE), :], v_ref[pl.ds(i * TILE, TILE), :], 0, 0)
        for i in range(tiles)
    ]
    for bit in range(inner):
        for i in range(tiles):
            place = (i >> bit) ^ 1
            value = nodes[place].astype(BF16) if (i >> bit) & 1 else jnp.zeros((head_dim, head_dim), BF16)
            sib_ref[i, :, pl.ds(bit * head_dim, head_dim)] = value
        nodes = [nodes[2 * i] + nodes[2 * i + 1] for i in range(len(nodes) // 2)]
    state_ref[...] = nodes[0].astype(BF16)


    def local_tile(i):
        rows = pl.ds(pl.multiple_of(i * TILE, TILE), TILE)
        row_ids = lax.broadcasted_iota(jnp.int32, (table.shape[1], TILE), 0)
        onehot = (row_ids == ids_ref[:, rows]).astype(F32).astype(BF16)
        coeff = dot(jnp.concatenate([onehot] * 3, axis=0), table3, 0, 1)
        coeff_ref[rows, :] = coeff
        levels = levels_ref[...]
        weights = jnp.zeros((TILE, TILE), F32)
        for level in range(tile_bits + 1):
            weights = jnp.where(levels == level, coeff[:, level : level + 1], weights)
        query = q_ref[rows, :]
        scores = dot(query, k_ref[rows, :], 1, 1)
        total = dot((weights * scores).astype(BF16), v_ref[rows, :], 1, 0)
        readout = dot(query, sib_ref[i], 1, 0)
        for bit in range(inner):
            level = tile_bits + 1 + bit
            total += coeff[:, level : level + 1] * readout[:, bit * head_dim : (bit + 1) * head_dim]
        total_ref[rows, :] = total

    def local_tiles(start, stop):
        def one(i, carry):
            local_tile(tile_of(head, i))
            return carry

        lax.fori_loop(start, stop, one, 0, unroll=True)

    with jax.named_scope("barrier"):
        pl.semaphore_wait(barrier, n_seq - 1 + jnp.minimum(head, 1) + jnp.minimum(last - head, 1))

    def state_copy(target):
        return pltpu.make_async_remote_copy(
            src_ref=state_ref, dst_ref=states_ref.at[seq],
            send_sem=state_send.at[0], recv_sem=state_recv.at[0],
            device_id=(target, head), device_id_type=MESH,
        )

    def partner(k):
        place = 0
        for bit in range(seq_bits):
            mine = lax.rem(seq // 2**bit, 2)
            place += 2**bit * (1 - mine if (k >> bit) & 1 else mine)
        return place

    for k in range(n_seq - 1, 0, -1):
        @pl.when(seq < partner(k))
        def _():
            state_copy(partner(k)).start()

    right, left = lax.rem(head + 1, n_head), lax.rem(head + n_head - 1, n_head)
    neighbours = (right, left)
    places = (head, last - head)

    half = n_head // 2
    spare = tiles - keep

    def origin_of(way, distance):
        return head - distance if way == 0 else head + distance

    def upward(origin):
        inside = jnp.logical_and(origin > 0, origin < half)
        return jnp.logical_or(inside, origin == last)

    def tile_of(origin, i):
        return jnp.where(upward(origin), i, tiles - 1 - i)

    def quad_of(origin, j):
        return jnp.where(upward(origin), j, quads - 1 - j)

    def kept(way, c):
        return c >= spare if way == 0 else c < keep

    def kept_quad(way, q):
        return 4 * q + 3 >= spare if way == 0 else 4 * q < keep

    def help_copy(way, i):
        return pltpu.make_async_remote_copy(
            src_ref=cot_hbm.at[pl.ds(i * TILE if way == 0 else (keep + i) * TILE, TILE), :],
            dst_ref=help_ref.at[pl.ds(i * TILE, TILE), :],
            send_sem=help_send.at[0], recv_sem=help_recv.at[0],
            device_id=(seq, left if way == 0 else right), device_id_type=MESH,
        )

    for way in range(2):
        @pl.when(places[way] == last)
        def _():
            for i in range(spare):
                help_copy(way, i).start()

    loads[4].wait()
    with jax.named_scope("local1"):
        local_tiles(0, ahead)
    acc_ref[...] = jnp.zeros_like(acc_ref)
    for way in range(2):
        blank = range(spare // 4 * 4, spare) if way == 0 else range(keep, (keep + 3) // 4 * 4)

        @pl.when(places[way] == last)
        def _():
            for c in blank:
                for origin in range(n_head):
                    @pl.when(origin != head)
                    def _():
                        gather_ref[origin, c] = jnp.zeros((head_dim, TILE), BF16)

    with jax.named_scope("states"):
        for block in range(1, n_seq):
            @pl.when(seq == block)
            def _():
                arrived = states_ref.at[pl.ds(0, block)]
                pltpu.make_async_remote_copy(
                    src_ref=arrived, dst_ref=arrived,
                    send_sem=state_send.at[0], recv_sem=state_recv.at[0],
                    device_id=(0, head), device_id_type=MESH,
                ).wait_recv()

    for bit in range(seq_bits):
        span = 2**bit
        node = seq // span
        columns = pl.ds(bit * head_dim, head_dim)

        @pl.when(lax.rem(node, 2) == 1)
        def _():
            total = jnp.zeros((head_dim, head_dim), F32)
            for offset in range(span):
                total += states_ref[(node - 1) * span + offset].astype(F32)
            upper = total.astype(BF16)
            flat_ref[pl.ds(0, head_dim), columns] = upper
            flat_ref[pl.ds(head_dim, head_dim), columns] = (total - upper.astype(F32)).astype(BF16)

        @pl.when(lax.rem(node, 2) == 0)
        def _():
            flat_ref[:, columns] = jnp.zeros((2 * head_dim, head_dim), BF16)

    def ring_copy(way, origin, c):
        return pltpu.make_async_remote_copy(
            src_ref=gather_ref.at[origin, c], dst_ref=gather_ref.at[origin, c],
            send_sem=ring_send.at[way], recv_sem=ring_recv.at[origin - way, c],
            device_id=(seq, neighbours[way]), device_id_type=MESH,
        )

    def passes(way, c):
        place = places[way]
        return jnp.logical_or(place + 1 < last, jnp.logical_and(place < last, kept(way, c)))

    def relay(way, distance, i):
        origin = origin_of(way, distance)
        c = tile_of(origin, i)
        ring_copy(way, origin, c).wait_recv()

        @pl.when(passes(way, c))
        def _():
            ring_copy(way, origin, c).start()

    def attn_tile(i):
        rows = pl.ds(pl.multiple_of(i * TILE, TILE), TILE)
        query = q_ref[rows, :]
        readout = dot(jnp.concatenate([query, query], axis=1), flat_ref[...], 1, 0)
        coeff = coeff_ref[rows, :]
        cross = jnp.zeros((TILE, head_dim), F32)
        for bit in range(seq_bits):
            level = local_bits + 1 + bit
            cross += coeff[:, level : level + 1] * readout[:, bit * head_dim : (bit + 1) * head_dim]
        total = total_ref[rows, :] + cross
        normed = total * lax.rsqrt(jnp.mean(total * total, axis=1, keepdims=True) + EPSILON)
        attn_ref[rows, :] = normed.astype(BF16)
        gather_ref[head, i] = normed.T.astype(BF16)

    def middle(way):
        return jnp.logical_and(places[way] >= 2, places[way] < last)

    early_tiles = BURST * spare

    def produce(local, relaying):
        def step(t, carry):
            tile = tile_of(head, t)
            attn_tile(tile)
            if local:
                local_tile(tile_of(head, t + ahead - lead))
            for way in range(2):
                @pl.when(passes(way, tile))
                def _():
                    ring_copy(way, head, tile).start()
            if relaying:
                for way in range(2):
                    @pl.when(jnp.logical_and(middle(way), t >= keep))
                    def _():
                        for i in range(BURST):
                            relay(way, 1, BURST * (t - keep) + i)
            return carry
        return step

    with jax.named_scope("phase1o"):
        lax.fori_loop(0, lead, produce(False, False), 0)
    with jax.named_scope("phase1a"):
        lax.fori_loop(lead, tiles - ahead + lead, produce(True, True), 0)
    with jax.named_scope("phase1b"):
        lax.fori_loop(tiles - ahead + lead, tiles, produce(False, True), 0)

    def joined(origin, q):
        return jnp.concatenate([gather_ref[origin, 4 * q + i] for i in range(4)], axis=1)

    def multiply(origin, q):
        rows = pl.ds(pl.multiple_of(q * (4 * TILE), 4 * TILE), 4 * TILE)
        acc_ref[origin] += dot(joined(origin, q), cot_ref[rows, :], 1, 0)

    def multiply_help(way, origin):
        base = 0 if way == 0 else keep
        for start in range(0, spare, 4):
            group = range(start, min(start + 4, spare))
            block = jnp.concatenate([gather_ref[origin, base + i] for i in group], axis=1)
            rows = help_ref[start * TILE : (group[-1] + 1) * TILE, :]
            acc_ref[n_head + origin] += dot(block, rows, 1, 0)

    def share_copy(slot, k):
        target = partner(k)
        return pltpu.make_async_remote_copy(
            src_ref=share_ref.at[slot, pl.ds(pl.multiple_of(target * rows_per, rows_per), rows_per), :],
            dst_ref=shares_ref.at[slot, k - 1],
            send_sem=share_send.at[slot], recv_sem=share_recv.at[slot],
            device_id=(target, head), device_id_type=MESH,
        )

    def send_share(slot):
        share_ref[slot] = (acc_ref[slot] * scale).astype(BF16)
        for k in range(n_seq - 1, 0, -1):
            if reducers == n_seq:
                share_copy(slot, k).start()
            else:
                pl.when(partner(k) < reducers)(lambda: share_copy(slot, k).start())

    def final_copy(slot, block, origin, kind, owner):
        columns = pl.ds(owner * piece if piece < width else 0, piece)
        return pltpu.make_async_remote_copy(
            src_ref=final_ref.at[slot, :, columns] if piece < width else final_ref.at[slot],
            dst_ref=finals_ref.at[kind, pl.ds(pl.multiple_of(seq * rows_per, rows_per), rows_per), :],
            send_sem=final_send.at[slot], recv_sem=final_recv.at[kind],
            device_id=(block * owners + owner, origin), device_id_type=MESH,
        )

    def is_self(block, origin, owner):
        return jnp.logical_and(block * owners + owner == seq, origin == head)

    def reduce_share(slot, block, origin, kind):
        @pl.when(seq < reducers)
        def _():
            mine = pl.ds(pl.multiple_of(seq * rows_per, rows_per), rows_per)
            arrived = shares_ref.at[slot]
            pltpu.make_async_remote_copy(
                src_ref=arrived, dst_ref=arrived,
                send_sem=share_send.at[slot], recv_sem=share_recv.at[slot],
                device_id=(0, head), device_id_type=MESH,
            ).wait_recv()
            whole = acc_ref[slot, mine, :] * scale
            for source in range(n_seq - 1):
                whole += shares_ref[slot, source].astype(F32)
            final_ref[slot] = whole.astype(BF16)
            for owner in range(owners):
                @pl.when(jnp.logical_not(is_self(block, origin, owner)))
                def _():
                    final_copy(slot, block, origin, kind, owner).start()

                @pl.when(is_self(block, origin, owner))
                def _():
                    start = owner * piece if piece < width else 0
                    finals_ref[kind, mine, :] = final_ref[slot, :, pl.ds(start, piece)]

    loads[5].wait()

    def arrive(way, origin, q):
        for c in range(4):
            @pl.when(kept(way, 4 * q + c))
            def _():
                ring_copy(way, origin, 4 * q + c).wait_recv()

    def helper(way):
        return jnp.logical_and(places[way] == last - 1, helps)

    def block_of(way):
        return last if way == 0 else 0

    def every_group(distance, act):
        @pl.when(distance == 0)
        def _():
            act(head, head, head, 0)
            if helps:
                for way in range(2):
                    pl.when(helper(way))(functools.partial(act, n_head + head, block_of(way), head, 1))

        for way in range(2):
            origin = origin_of(way, distance)

            @pl.when(jnp.logical_and(distance > 0, distance < places[way]))
            def _():
                act(origin, head, origin, 0)
                if helps:
                    pl.when(helper(way))(functools.partial(act, n_head + origin, block_of(way), origin, 1))

    began = early_tiles
    if last > 3:
        began = tiles
        for way in range(2):
            def rest(i, carry):
                relay(way, 1, i)
                return carry

            def more(n, carry):
                relay(way, 2 + n // tiles, lax.rem(n, tiles))
                return carry

            @pl.when(middle(way))
            def _():
                lax.fori_loop(early_tiles, tiles, rest, 0)
                lax.fori_loop(0, (places[way] - 2) * tiles, more, 0)

    farthest = jnp.maximum(places[0], places[1])

    def flow(u, carry):
        for way in range(2):
            place, origin = places[way], block_of(1 - way)
            i = u - 1 - LAG * (place - 1)

            if began < tiles:
                @pl.when(jnp.logical_and(middle(way), u < tiles - began))
                def _():
                    relay(way, 1, began + u)

            @pl.when(jnp.logical_and(jnp.logical_and(place > 0, place < last), jnp.logical_and(i >= 0, i < tiles)))
            def _():
                relay(way, place, i)

        for way in range(2):
            place, origin = places[way], block_of(1 - way)
            i = u - 1 - LAG * (place - 1)
            j = i // 4
            q = quad_of(origin, j)

            @pl.when(jnp.logical_and(jnp.logical_and(place > 0, i - 4 * j == 3), jnp.logical_and(i >= 0, i < tiles)))
            def _():
                @pl.when(jnp.logical_or(place < last, kept_quad(way, q)))
                def _():
                    pl.when(place == last)(functools.partial(arrive, way, origin, q))
                    multiply(origin, q)
                done = jnp.where(place == last, (keep + 3) // 4 - 1, quads - 1)
                pl.when(j == done)(functools.partial(send_share, origin))
                if helps:
                    @pl.when(jnp.logical_and(helper(way), j == quads - 1))
                    def _():
                        multiply_help(way, origin)
                        send_share(n_head + origin)

        distance = u // quads
        j = u - quads * distance

        @pl.when(distance == 0)
        def _():
            multiply(head, quad_of(head, j))

        for way in range(2):
            place, origin = places[way], origin_of(way, distance)
            q = quad_of(origin, j)

            @pl.when(jnp.logical_and(jnp.logical_and(distance > 0, distance < place), jnp.logical_or(place < last, kept_quad(way, q))))
            def _():
                pl.when(place == last)(functools.partial(arrive, way, origin, q))
                multiply(origin, q)

            if helps:
                @pl.when(jnp.logical_and(helper(way), jnp.logical_and(distance < place, j == quads - 1)))
                def _():
                    @pl.when(distance == 0)
                    def _():
                        pltpu.make_async_remote_copy(
                            src_ref=help_ref, dst_ref=help_ref,
                            send_sem=help_send.at[0], recv_sem=help_recv.at[0],
                            device_id=(seq, left if way == 0 else right), device_id_type=MESH,
                        ).wait_recv()
                    multiply_help(way, origin)

        @pl.when(j == quads - 1)
        def _():
            every_group(distance, lambda slot, *_: send_share(slot))
            pl.when(jnp.logical_and(farthest == last, distance >= 2))(lambda: every_group(distance - 2, reduce_share))
        return carry

    with jax.named_scope("flow"):
        lax.fori_loop(0, jnp.maximum(tiles + 1 + LAG * (farthest - 1), quads * (farthest + 2)), flow, 0)

    ends = []
    for way in range(2):
        place, origin = places[way], block_of(1 - way)
        if helps:
            ends.append((helper(way), n_head + origin, block_of(way), origin, 1))
    for way in range(2):
        place, origin = places[way], block_of(1 - way)
        ends.append((place > 0, origin, head, origin, 0))
    with jax.named_scope("reducelast"):
        @pl.when(farthest < last)
        def _():
            def one(distance, carry):
                every_group(distance, reduce_share)
                return carry

            lax.fori_loop(0, farthest, one, 0)

        for condition, *rest in ends[:-2]:
            pl.when(condition)(functools.partial(reduce_share, *rest))
        closer = places[0] <= places[1]
        for flip, pair in ((closer, ends[-2:]), (jnp.logical_not(closer), ends[-2:][::-1])):
            @pl.when(flip)
            def _():
                for condition, *rest in pair:
                    pl.when(condition)(functools.partial(reduce_share, *rest))

    with jax.named_scope("finals"):
        home = seq // owners
        at_end = jnp.logical_and(jnp.logical_or(home == 0, home == last), head != home)
        for kind in range(2 if helps else 1):
            plane = home if kind == 0 else jnp.where(home == 0, 1, last - 1)
            own = jnp.logical_and(seq < reducers, head == plane)
            expected = at_end if kind else seq >= 0
            for count, match in ((reducers - 1, own), (reducers, jnp.logical_not(own))):
                @pl.when(jnp.logical_and(expected, match))
                def _():
                    arrived = finals_ref.at[kind, pl.ds(0, count * rows_per), :]
                    pltpu.make_async_remote_copy(
                        src_ref=arrived, dst_ref=arrived,
                        send_sem=final_send.at[0], recv_sem=final_recv.at[kind],
                        device_id=(0, plane), device_id_type=MESH,
                    ).wait_recv()
        whole_ref[...] = finals_ref[0].astype(F32)
        if helps:
            @pl.when(at_end)
            def _():
                whole_ref[...] += finals_ref[1].astype(F32)
        per = grad_ref.shape[1]
        if per == piece:
            grad_ref[...] = whole_ref[...]
        else:
            for owner in range(owners):
                @pl.when(lax.rem(seq, owners) == owner)
                def _():
                    grad_ref[...] = whole_ref[:, owner * per : (owner + 1) * per]

    with jax.named_scope("drain"):
        for block in range(n_seq - 1):
            @pl.when(seq == block)
            def _():
                sent = states_ref.at[pl.ds(0, n_seq - 1 - block)]
                pltpu.make_async_remote_copy(
                    src_ref=sent, dst_ref=sent,
                    send_sem=state_send.at[0], recv_sem=state_recv.at[0],
                    device_id=(0, head), device_id_type=MESH,
                ).wait_send()
        for way in range(2):
            if helps:
                @pl.when(places[way] == last)
                def _():
                    pltpu.make_async_remote_copy(
                        src_ref=help_ref, dst_ref=help_ref,
                        send_sem=help_send.at[0], recv_sem=help_recv.at[0],
                        device_id=(seq, left if way == 0 else right), device_id_type=MESH,
                    ).wait_send()
            for place in range(last):
                @pl.when(places[way] == place)
                def _():
                    count = tiles if place + 1 < last else keep
                    sent = gather_ref.at[pl.ds(0, place + 1), pl.ds(0, count)]
                    pltpu.make_async_remote_copy(
                        src_ref=sent, dst_ref=sent,
                        send_sem=ring_send.at[way], recv_sem=ring_recv.at[0, 0],
                        device_id=(seq, neighbours[way]), device_id_type=MESH,
                    ).wait_send()
        def drain(slot, block, origin, kind):
            def sent_shares(count):
                sent = share_ref.at[slot, pl.ds(0, count * rows_per), :]
                pltpu.make_async_remote_copy(
                    src_ref=sent, dst_ref=sent,
                    send_sem=share_send.at[slot], recv_sem=share_recv.at[slot],
                    device_id=(0, head), device_id_type=MESH,
                ).wait_send()

            def sent_finals(count):
                sent = finals_ref.at[0, pl.ds(0, count * rows_per), :]
                pltpu.make_async_remote_copy(
                    src_ref=sent, dst_ref=sent,
                    send_sem=final_send.at[slot], recv_sem=final_recv.at[0],
                    device_id=(0, head), device_id_type=MESH,
                ).wait_send()

            pl.when(seq < reducers)(lambda: sent_shares(reducers - 1))
            if reducers < n_seq:
                pl.when(seq >= reducers)(lambda: sent_shares(reducers))
            near = jnp.logical_and(seq // owners == block, origin == head)
            pl.when(jnp.logical_and(seq < reducers, jnp.logical_not(near)))(lambda: sent_finals(owners))
            if owners > 1:
                pl.when(jnp.logical_and(seq < reducers, near))(lambda: sent_finals(owners - 1))

        for origin in range(n_head):
            drain(origin, head, origin, 0)
        if helps:
            for way in range(2):
                for origin in range(n_head):
                    @pl.when(jnp.logical_and(helper(way), origin != block_of(way)))
                    def _():
                        drain(n_head + origin, block_of(way), origin, 1)


def finish(attn_ref, grad_ref, attn_out, grad_out, turned_ref, sem):
    attn_copy = pltpu.make_async_copy(attn_ref, attn_out, sem.at[0])
    attn_copy.start()
    turned_ref[...] = grad_ref[...].T
    grad_copy = pltpu.make_async_copy(turned_ref, grad_out, sem.at[1])
    grad_copy.start()
    attn_copy.wait()
    grad_copy.wait()


def body(n_seq, n_head, queries, keys, values, level_ids, level_table, out_cotangent):
    block_len, head_dim = queries.shape
    width = out_cotangent.shape[1]
    per = width * n_head // n_seq
    piece = per if per % 128 == 0 else width
    seq_bits = n_seq.bit_length() - 1
    tiles = block_len // TILE
    inner = tiles.bit_length() - 1
    rows_per = max(16, head_dim // n_seq)
    slots = 2 * n_head
    spare = max(4, tiles - kept_tiles(n_head, tiles))
    dma = pltpu.SemaphoreType.DMA
    vmem = pl.BlockSpec(memory_space=pltpu.VMEM)
    hbm = pl.BlockSpec(memory_space=pltpu.HBM)
    attn_out, grad = pl.pallas_call(
        functools.partial(kernel, n_seq, n_head),
        out_shape=(
            pltpu.VMEM((block_len, head_dim), BF16),
            pltpu.VMEM((head_dim, per), F32),
        ),
        in_specs=[hbm] * 6,
        out_specs=(vmem, vmem),
        scratch_shapes=[
            pltpu.VMEM((block_len, head_dim), BF16),
            pltpu.VMEM((block_len, head_dim), BF16),
            pltpu.VMEM((block_len, head_dim), BF16),
            pltpu.VMEM((block_len, width), BF16),
            pltpu.VMEM((1, block_len), jnp.int32),
            pltpu.VMEM(level_table.shape[::-1], F32),
            pltpu.VMEM((TILE, TILE), jnp.int32),
            pltpu.VMEM((block_len, level_table.shape[1]), F32),
            pltpu.VMEM((block_len, head_dim), F32),
            pltpu.VMEM((tiles, head_dim, inner * head_dim), BF16),
            pltpu.VMEM((head_dim, head_dim), BF16),
            pltpu.VMEM((n_seq, head_dim, head_dim), BF16),
            pltpu.VMEM((2 * head_dim, seq_bits * head_dim), BF16),
            pltpu.VMEM((n_head, tiles, head_dim, TILE), BF16),
            pltpu.VMEM((slots, head_dim, width), F32),
            pltpu.VMEM((slots, head_dim, width), BF16),
            pltpu.VMEM((slots, n_seq - 1, rows_per, width), BF16),
            pltpu.VMEM((slots, rows_per, width), BF16),
            pltpu.VMEM((2, head_dim, piece), BF16),
            pltpu.VMEM((head_dim, piece), F32),
            pltpu.VMEM((spare * TILE, width), BF16),
            dma((6,)),
            dma((1,)),
            dma((1,)),
            dma((2,)),
            dma((max(1, n_head - 1), tiles)),
            dma((slots,)),
            dma((slots,)),
            dma((slots,)),
            dma((2,)),
            dma((1,)),
            dma((1,)),
        ],
        compiler_params=pltpu.CompilerParams(
            collective_id=0, has_side_effects=True, vmem_limit_bytes=60 * 2**20
        ),
    )(queries, keys, values, level_ids[None, :], level_table.T, out_cotangent)
    return pl.pallas_call(
        finish,
        out_shape=(
            jax.ShapeDtypeStruct((block_len, head_dim), BF16),
            jax.ShapeDtypeStruct((per, head_dim), F32),
        ),
        in_specs=[vmem, vmem],
        out_specs=(hbm, hbm),
        scratch_shapes=[pltpu.VMEM((per, head_dim), F32), dma((2,))],
        compiler_params=pltpu.CompilerParams(vmem_limit_bytes=4 * 2**20),
    )(attn_out, grad)


def solution(mesh):
    in_specs = (
        P("seq", "head"),
        P("seq", "head"),
        P("seq", "head"),
        P("seq"),
        P(),
        P("seq", "head"),
    )
    out_specs = (P("seq", "head"), P("seq", "head"))
    return jax.shard_map(
        functools.partial(body, mesh.shape["seq"], mesh.shape["head"]),
        mesh=mesh, in_specs=in_specs, out_specs=out_specs, check_vma=False,
    )
```

```python
import functools

import jax
import jax.numpy as jnp
from jax import lax
from jax.experimental import pallas as pl
from jax.experimental.pallas import tpu as pltpu
from jax.sharding import PartitionSpec as P

EPSILON = 1e-06
TILE = 128
KEEP = 11
AHEAD = 8
LEAD = 6
LAG = 6
SETTLED = 12
BURST = 2
MESH = pl.DeviceIdType.MESH
F32 = jnp.float32
BF16 = jnp.bfloat16


def dot(a, b, ca, cb):
    return lax.dot_general(a, b, (((ca,), (cb,)), ((), ())), preferred_element_type=F32)


def tile_levels(tile):
    row = lax.broadcasted_iota(jnp.int32, (tile, tile), 0)
    col = lax.broadcasted_iota(jnp.int32, (tile, tile), 1)
    apart = jnp.bitwise_xor(row, col)
    levels = jnp.zeros((tile, tile), jnp.int32)
    for bit in range(tile.bit_length() - 1):
        levels = levels + (jnp.right_shift(apart, bit) > 0).astype(jnp.int32)
    return jnp.where(col <= row, levels, -1)


def kept_tiles(n_head, tiles):
    return tiles * KEEP // 16 if n_head >= 4 else tiles


def kernel(
    n_seq, n_head,
    q_hbm, k_hbm, v_hbm, ids_hbm, table_hbm, cot_hbm,
    attn_ref, grad_ref,
    q_ref, k_ref, v_ref, cot_ref, ids_ref, table_ref, levels_ref, coeff_ref, total_ref, sib_ref,
    state_ref, states_ref, flat_ref, gather_ref, acc_ref,
    share_ref, shares_ref, final_ref, finals_ref, whole_ref, help_ref,
    load_sem, state_send, state_recv, ring_send, ring_recv,
    share_send, share_recv, final_send, final_recv, help_send, help_recv,
):
    seq, head = lax.axis_index("seq"), lax.axis_index("head")
    block_len, head_dim = q_ref.shape
    width = cot_ref.shape[1]
    tiles = block_len // TILE
    pairs = tiles // 2
    tile_bits = TILE.bit_length() - 1
    local_bits = block_len.bit_length() - 1
    inner = local_bits - tile_bits
    seq_bits = n_seq.bit_length() - 1
    owners = n_seq // n_head
    rows_per = max(16, head_dim // n_seq)
    reducers = head_dim // rows_per
    piece = finals_ref.shape[2]
    last = n_head - 1
    keep = kept_tiles(n_head, tiles)
    helps = keep < tiles
    quads = tiles // 4
    ahead = min(AHEAD, tiles)
    lead = min(LEAD, ahead)
    scale = (block_len * n_seq) ** (-0.5)

    loads = [
        pltpu.make_async_copy(src, dst, load_sem.at[i])
        for i, (src, dst) in enumerate(
            [
                (k_hbm, k_ref), (v_hbm, v_ref), (table_hbm, table_ref), (ids_hbm, ids_ref),
                (q_hbm, q_ref), (cot_hbm, cot_ref),
            ]
        )
    ]
    for load in loads[:4]:
        load.start()

    barrier = pltpu.get_barrier_semaphore()

    def greet(device):
        pl.semaphore_signal(barrier, inc=1, device_id=device, device_id_type=MESH)

    for step in range(1, n_seq):
        greet((lax.rem(seq + step, n_seq), head))
    pl.when(head > 0)(lambda: greet((seq, head - 1)))
    pl.when(head < n_head - 1)(lambda: greet((seq, head + 1)))

    levels_ref[...] = tile_levels(TILE)
    right, left = lax.rem(head + 1, n_head), lax.rem(head + n_head - 1, n_head)
    neighbours = (right, left)
    places = (head, last - head)

    half = n_head // 2
    spare = tiles - keep

    def origin_of(way, distance):
        return head - distance if way == 0 else head + distance

    def upward(origin):
        inside = jnp.logical_and(origin > 0, origin < half)
        return jnp.logical_or(inside, origin == last)

    def tile_of(origin, i):
        return jnp.where(upward(origin), i, tiles - 1 - i)

    def quad_of(origin, j):
        return jnp.where(upward(origin), j, quads - 1 - j)

    def kept(way, c):
        return c >= spare if way == 0 else c < keep

    def kept_quad(way, q):
        return 4 * q + 3 >= spare if way == 0 else 4 * q < keep

    def help_copy(way, i):
        return pltpu.make_async_remote_copy(
            src_ref=cot_hbm.at[pl.ds(i * TILE if way == 0 else (keep + i) * TILE, TILE), :],
            dst_ref=help_ref.at[pl.ds(i * TILE, TILE), :],
            send_sem=help_send.at[0], recv_sem=help_recv.at[0],
            device_id=(seq, left if way == 0 else right), device_id_type=MESH,
        )

    at_edge = jnp.logical_or(head == 0, head == last)

    def meet():
        pl.semaphore_wait(barrier, n_seq - 1 + jnp.minimum(head, 1) + jnp.minimum(last - head, 1))

    @pl.when(at_edge)
    def _():
        meet()
        for way in range(2):
            @pl.when(places[way] == last)
            def _():
                for i in range(spare):
                    help_copy(way, i).start()

    with jax.named_scope("kv"):
        for load in loads[:4]:
            load.wait()
    for load in loads[4:]:
        load.start()
    table = table_ref[...]
    high = table.astype(BF16)
    rest = table - high.astype(F32)
    mid = rest.astype(BF16)
    low = (rest - mid.astype(F32)).astype(BF16)
    table3 = jnp.concatenate([high, mid, low], axis=1)

    nodes = [
        dot(k_ref[pl.ds(i * TILE, TILE), :], v_ref[pl.ds(i * TILE, TILE), :], 0, 0)
        for i in range(tiles)
    ]
    for bit in range(inner):
        for i in range(tiles):
            place = (i >> bit) ^ 1
            value = nodes[place].astype(BF16) if (i >> bit) & 1 else jnp.zeros((head_dim, head_dim), BF16)
            sib_ref[i, :, pl.ds(bit * head_dim, head_dim)] = value
        nodes = [nodes[2 * i] + nodes[2 * i + 1] for i in range(len(nodes) // 2)]
    state_ref[...] = nodes[0].astype(BF16)


    def local_tile(i):
        rows = pl.ds(pl.multiple_of(i * TILE, TILE), TILE)
        row_ids = lax.broadcasted_iota(jnp.int32, (table.shape[1], TILE), 0)
        onehot = (row_ids == ids_ref[:, rows]).astype(F32).astype(BF16)
        coeff = dot(jnp.concatenate([onehot] * 3, axis=0), table3, 0, 1)
        coeff_ref[rows, :] = coeff
        levels = levels_ref[...]
        weights = jnp.zeros((TILE, TILE), F32)
        for level in range(tile_bits + 1):
            weights = jnp.where(levels == level, coeff[:, level : level + 1], weights)
        query = q_ref[rows, :]
        scores = dot(query, k_ref[rows, :], 1, 1)
        total = dot((weights * scores).astype(BF16), v_ref[rows, :], 1, 0)
        readout = dot(query, sib_ref[i], 1, 0)
        for bit in range(inner):
            level = tile_bits + 1 + bit
            total += coeff[:, level : level + 1] * readout[:, bit * head_dim : (bit + 1) * head_dim]
        total_ref[rows, :] = total

    def local_tiles(start, stop):
        def one(i, carry):
            local_tile(tile_of(head, i))
            return carry

        lax.fori_loop(start, stop, one, 0, unroll=True)

    with jax.named_scope("barrier"):
        pl.when(jnp.logical_not(at_edge))(meet)

    def state_copy(target):
        return pltpu.make_async_remote_copy(
            src_ref=state_ref, dst_ref=states_ref.at[seq],
            send_sem=state_send.at[0], recv_sem=state_recv.at[0],
            device_id=(target, head), device_id_type=MESH,
        )

    def partner(k):
        place = 0
        for bit in range(seq_bits):
            mine = lax.rem(seq // 2**bit, 2)
            place += 2**bit * (1 - mine if (k >> bit) & 1 else mine)
        return place

    for k in range(n_seq - 1, 0, -1):
        @pl.when(seq < partner(k))
        def _():
            state_copy(partner(k)).start()

    loads[4].wait()
    with jax.named_scope("local1"):
        local_tiles(0, ahead)
    acc_ref[...] = jnp.zeros_like(acc_ref)
    for way in range(2):
        blank = range(spare // 4 * 4, spare) if way == 0 else range(keep, (keep + 3) // 4 * 4)

        @pl.when(places[way] == last)
        def _():
            for c in blank:
                for origin in range(n_head):
                    @pl.when(origin != head)
                    def _():
                        gather_ref[origin, c] = jnp.zeros((head_dim, TILE), BF16)

    with jax.named_scope("states"):
        for block in range(1, n_seq):
            @pl.when(seq == block)
            def _():
                arrived = states_ref.at[pl.ds(0, block)]
                pltpu.make_async_remote_copy(
                    src_ref=arrived, dst_ref=arrived,
                    send_sem=state_send.at[0], recv_sem=state_recv.at[0],
                    device_id=(0, head), device_id_type=MESH,
                ).wait_recv()

    for bit in range(seq_bits):
        span = 2**bit
        node = seq // span
        columns = pl.ds(bit * head_dim, head_dim)

        @pl.when(lax.rem(node, 2) == 1)
        def _():
            total = jnp.zeros((head_dim, head_dim), F32)
            for offset in range(span):
                total += states_ref[(node - 1) * span + offset].astype(F32)
            upper = total.astype(BF16)
            flat_ref[pl.ds(0, head_dim), columns] = upper
            flat_ref[pl.ds(head_dim, head_dim), columns] = (total - upper.astype(F32)).astype(BF16)

        @pl.when(lax.rem(node, 2) == 0)
        def _():
            flat_ref[:, columns] = jnp.zeros((2 * head_dim, head_dim), BF16)

    def ring_copy(way, origin, c):
        return pltpu.make_async_remote_copy(
            src_ref=gather_ref.at[origin, c], dst_ref=gather_ref.at[origin, c],
            send_sem=ring_send.at[way], recv_sem=ring_recv.at[origin - way, c],
            device_id=(seq, neighbours[way]), device_id_type=MESH,
        )

    def passes(way, c):
        place = places[way]
        return jnp.logical_or(place + 1 < last, jnp.logical_and(place < last, kept(way, c)))

    def relay(way, distance, i):
        origin = origin_of(way, distance)
        c = tile_of(origin, i)
        ring_copy(way, origin, c).wait_recv()

        @pl.when(passes(way, c))
        def _():
            ring_copy(way, origin, c).start()

    def attn_tile(i):
        rows = pl.ds(pl.multiple_of(i * TILE, TILE), TILE)
        query = q_ref[rows, :]
        readout = dot(jnp.concatenate([query, query], axis=1), flat_ref[...], 1, 0)
        coeff = coeff_ref[rows, :]
        cross = jnp.zeros((TILE, head_dim), F32)
        for bit in range(seq_bits):
            level = local_bits + 1 + bit
            cross += coeff[:, level : level + 1] * readout[:, bit * head_dim : (bit + 1) * head_dim]
        total = total_ref[rows, :] + cross
        normed = total * lax.rsqrt(jnp.mean(total * total, axis=1, keepdims=True) + EPSILON)
        attn_ref[rows, :] = normed.astype(BF16)
        gather_ref[head, i] = normed.T.astype(BF16)

    def middle(way):
        return jnp.logical_and(places[way] >= 2, places[way] < last)

    early_tiles = BURST * spare

    def produce(local, relaying):
        def step(t, carry):
            tile = tile_of(head, t)
            attn_tile(tile)
            if local:
                local_tile(tile_of(head, t + ahead - lead))
            for way in range(2):
                @pl.when(passes(way, tile))
                def _():
                    ring_copy(way, head, tile).start()
            if relaying:
                for way in range(2):
                    @pl.when(jnp.logical_and(middle(way), t >= keep))
                    def _():
                        for i in range(BURST):
                            relay(way, 1, BURST * (t - keep) + i)
            return carry
        return step

    with jax.named_scope("phase1o"):
        lax.fori_loop(0, lead, produce(False, False), 0)
    with jax.named_scope("phase1a"):
        lax.fori_loop(lead, tiles - ahead + lead, produce(True, True), 0)
    with jax.named_scope("phase1b"):
        lax.fori_loop(tiles - ahead + lead, tiles, produce(False, True), 0)

    def joined(origin, q):
        return jnp.concatenate([gather_ref[origin, 4 * q + i] for i in range(4)], axis=1)

    def multiply(origin, q):
        rows = pl.ds(pl.multiple_of(q * (4 * TILE), 4 * TILE), 4 * TILE)
        acc_ref[origin] += dot(joined(origin, q), cot_ref[rows, :], 1, 0)

    def multiply_help(way, origin):
        base = 0 if way == 0 else keep
        for start in range(0, spare, 4):
            group = range(start, min(start + 4, spare))
            block = jnp.concatenate([gather_ref[origin, base + i] for i in group], axis=1)
            rows = help_ref[start * TILE : (group[-1] + 1) * TILE, :]
            acc_ref[n_head + origin] += dot(block, rows, 1, 0)

    def share_copy(slot, k):
        target = partner(k)
        return pltpu.make_async_remote_copy(
            src_ref=share_ref.at[slot, pl.ds(pl.multiple_of(target * rows_per, rows_per), rows_per), :],
            dst_ref=shares_ref.at[slot, k - 1],
            send_sem=share_send.at[slot], recv_sem=share_recv.at[slot],
            device_id=(target, head), device_id_type=MESH,
        )

    def send_share(slot):
        share_ref[slot] = (acc_ref[slot] * scale).astype(BF16)
        for k in range(n_seq - 1, 0, -1):
            if reducers == n_seq:
                share_copy(slot, k).start()
            else:
                pl.when(partner(k) < reducers)(lambda: share_copy(slot, k).start())

    def final_copy(slot, block, origin, kind, owner):
        columns = pl.ds(owner * piece if piece < width else 0, piece)
        return pltpu.make_async_remote_copy(
            src_ref=final_ref.at[slot, :, columns] if piece < width else final_ref.at[slot],
            dst_ref=finals_ref.at[kind, pl.ds(pl.multiple_of(seq * rows_per, rows_per), rows_per), :],
            send_sem=final_send.at[slot], recv_sem=final_recv.at[kind],
            device_id=(block * owners + owner, origin), device_id_type=MESH,
        )

    def is_self(block, origin, owner):
        return jnp.logical_and(block * owners + owner == seq, origin == head)

    def reduce_share(slot, block, origin, kind):
        @pl.when(seq < reducers)
        def _():
            mine = pl.ds(pl.multiple_of(seq * rows_per, rows_per), rows_per)
            arrived = shares_ref.at[slot]
            pltpu.make_async_remote_copy(
                src_ref=arrived, dst_ref=arrived,
                send_sem=share_send.at[slot], recv_sem=share_recv.at[slot],
                device_id=(0, head), device_id_type=MESH,
            ).wait_recv()
            whole = acc_ref[slot, mine, :] * scale
            for source in range(n_seq - 1):
                whole += shares_ref[slot, source].astype(F32)
            final_ref[slot] = whole.astype(BF16)
            for owner in range(owners):
                @pl.when(jnp.logical_not(is_self(block, origin, owner)))
                def _():
                    final_copy(slot, block, origin, kind, owner).start()

                @pl.when(is_self(block, origin, owner))
                def _():
                    start = owner * piece if piece < width else 0
                    finals_ref[kind, mine, :] = final_ref[slot, :, pl.ds(start, piece)]

    loads[5].wait()

    def arrive(way, origin, q):
        for c in range(4):
            @pl.when(kept(way, 4 * q + c))
            def _():
                ring_copy(way, origin, 4 * q + c).wait_recv()

    def helper(way):
        return jnp.logical_and(places[way] == last - 1, helps)

    def block_of(way):
        return last if way == 0 else 0

    def every_group(distance, act):
        @pl.when(distance == 0)
        def _():
            act(head, head, head, 0)
            if helps:
                for way in range(2):
                    pl.when(helper(way))(functools.partial(act, n_head + head, block_of(way), head, 1))

        for way in range(2):
            origin = origin_of(way, distance)

            @pl.when(jnp.logical_and(distance > 0, distance < places[way]))
            def _():
                act(origin, head, origin, 0)
                if helps:
                    pl.when(helper(way))(functools.partial(act, n_head + origin, block_of(way), origin, 1))

    began = early_tiles
    if last > 3:
        began = tiles
        for way in range(2):
            def rest(i, carry):
                relay(way, 1, i)
                return carry

            def more(n, carry):
                relay(way, 2 + n // tiles, lax.rem(n, tiles))
                return carry

            @pl.when(middle(way))
            def _():
                lax.fori_loop(early_tiles, tiles, rest, 0)
                lax.fori_loop(0, (places[way] - 2) * tiles, more, 0)

    farthest = jnp.maximum(places[0], places[1])

    def flow(u, carry):
        for way in range(2):
            place, origin = places[way], block_of(1 - way)
            i = u - 1 - LAG * (place - 1)

            if began < tiles:
                @pl.when(jnp.logical_and(middle(way), u < tiles - began))
                def _():
                    relay(way, 1, began + u)

            @pl.when(jnp.logical_and(jnp.logical_and(place > 0, place < last), jnp.logical_and(i >= 0, i < tiles)))
            def _():
                relay(way, place, i)

        for way in range(2):
            place, origin = places[way], block_of(1 - way)
            i = u - 1 - LAG * (place - 1)
            j = i // 4
            q = quad_of(origin, j)

            @pl.when(jnp.logical_and(jnp.logical_and(place > 0, i - 4 * j == 3), jnp.logical_and(i >= 0, i < tiles)))
            def _():
                @pl.when(jnp.logical_or(place < last, kept_quad(way, q)))
                def _():
                    pl.when(place == last)(functools.partial(arrive, way, origin, q))
                    multiply(origin, q)
                done = jnp.where(place == last, (keep + 3) // 4 - 1, quads - 1)
                pl.when(j == done)(functools.partial(send_share, origin))
                if helps:
                    @pl.when(jnp.logical_and(helper(way), j == quads - 1))
                    def _():
                        multiply_help(way, origin)
                        send_share(n_head + origin)

        distance = u // quads
        j = u - quads * distance

        @pl.when(distance == 0)
        def _():
            multiply(head, quad_of(head, j))

        for way in range(2):
            place, origin = places[way], origin_of(way, distance)
            q = quad_of(origin, j)

            @pl.when(jnp.logical_and(jnp.logical_and(distance > 0, distance < place), jnp.logical_or(place < last, kept_quad(way, q))))
            def _():
                pl.when(place == last)(functools.partial(arrive, way, origin, q))
                multiply(origin, q)

            if helps:
                @pl.when(jnp.logical_and(helper(way), jnp.logical_and(distance < place, j == quads - 1)))
                def _():
                    @pl.when(distance == 0)
                    def _():
                        pltpu.make_async_remote_copy(
                            src_ref=help_ref, dst_ref=help_ref,
                            send_sem=help_send.at[0], recv_sem=help_recv.at[0],
                            device_id=(seq, left if way == 0 else right), device_id_type=MESH,
                        ).wait_recv()
                    multiply_help(way, origin)

        @pl.when(j == quads - 1)
        def _():
            every_group(distance, lambda slot, *_: send_share(slot))

        behind = jnp.maximum(u - SETTLED, 0)

        @pl.when(jnp.logical_and(jnp.logical_and(u >= SETTLED, lax.rem(behind, quads) == 0), behind // quads < farthest))
        def _():
            every_group(behind // quads, reduce_share)
        return carry

    with jax.named_scope("flow"):
        lax.fori_loop(0, jnp.maximum(tiles + 1 + LAG * (farthest - 1), quads * (farthest - 1) + SETTLED + 1), flow, 0)

    ends = []
    for way in range(2):
        place, origin = places[way], block_of(1 - way)
        if helps:
            ends.append((helper(way), n_head + origin, block_of(way), origin, 1))
    for way in range(2):
        place, origin = places[way], block_of(1 - way)
        ends.append((place > 0, origin, head, origin, 0))
    with jax.named_scope("reducelast"):
        for condition, *rest in ends[:-2]:
            pl.when(condition)(functools.partial(reduce_share, *rest))
        closer = places[0] <= places[1]
        for flip, pair in ((closer, ends[-2:]), (jnp.logical_not(closer), ends[-2:][::-1])):
            @pl.when(flip)
            def _():
                for condition, *rest in pair:
                    pl.when(condition)(functools.partial(reduce_share, *rest))

    with jax.named_scope("finals"):
        home = seq // owners
        at_end = jnp.logical_and(jnp.logical_or(home == 0, home == last), head != home)
        for kind in range(2 if helps else 1):
            plane = home if kind == 0 else jnp.where(home == 0, 1, last - 1)
            own = jnp.logical_and(seq < reducers, head == plane)
            expected = at_end if kind else seq >= 0
            for count, match in ((reducers - 1, own), (reducers, jnp.logical_not(own))):
                @pl.when(jnp.logical_and(expected, match))
                def _():
                    arrived = finals_ref.at[kind, pl.ds(0, count * rows_per), :]
                    pltpu.make_async_remote_copy(
                        src_ref=arrived, dst_ref=arrived,
                        send_sem=final_send.at[0], recv_sem=final_recv.at[kind],
                        device_id=(0, plane), device_id_type=MESH,
                    ).wait_recv()
        whole_ref[...] = finals_ref[0].astype(F32)
        if helps:
            @pl.when(at_end)
            def _():
                whole_ref[...] += finals_ref[1].astype(F32)
        per = grad_ref.shape[1]
        if per == piece:
            grad_ref[...] = whole_ref[...]
        else:
            for owner in range(owners):
                @pl.when(lax.rem(seq, owners) == owner)
                def _():
                    grad_ref[...] = whole_ref[:, owner * per : (owner + 1) * per]

    with jax.named_scope("drain"):
        for block in range(n_seq - 1):
            @pl.when(seq == block)
            def _():
                sent = states_ref.at[pl.ds(0, n_seq - 1 - block)]
                pltpu.make_async_remote_copy(
                    src_ref=sent, dst_ref=sent,
                    send_sem=state_send.at[0], recv_sem=state_recv.at[0],
                    device_id=(0, head), device_id_type=MESH,
                ).wait_send()
        for way in range(2):
            if helps:
                @pl.when(places[way] == last)
                def _():
                    pltpu.make_async_remote_copy(
                        src_ref=help_ref, dst_ref=help_ref,
                        send_sem=help_send.at[0], recv_sem=help_recv.at[0],
                        device_id=(seq, left if way == 0 else right), device_id_type=MESH,
                    ).wait_send()
            for place in range(last):
                @pl.when(places[way] == place)
                def _():
                    count = tiles if place + 1 < last else keep
                    sent = gather_ref.at[pl.ds(0, place + 1), pl.ds(0, count)]
                    pltpu.make_async_remote_copy(
                        src_ref=sent, dst_ref=sent,
                        send_sem=ring_send.at[way], recv_sem=ring_recv.at[0, 0],
                        device_id=(seq, neighbours[way]), device_id_type=MESH,
                    ).wait_send()
        def drain(slot, block, origin, kind):
            def sent_shares(count):
                sent = share_ref.at[slot, pl.ds(0, count * rows_per), :]
                pltpu.make_async_remote_copy(
                    src_ref=sent, dst_ref=sent,
                    send_sem=share_send.at[slot], recv_sem=share_recv.at[slot],
                    device_id=(0, head), device_id_type=MESH,
                ).wait_send()

            def sent_finals(count):
                sent = finals_ref.at[0, pl.ds(0, count * rows_per), :]
                pltpu.make_async_remote_copy(
                    src_ref=sent, dst_ref=sent,
                    send_sem=final_send.at[slot], recv_sem=final_recv.at[0],
                    device_id=(0, head), device_id_type=MESH,
                ).wait_send()

            pl.when(seq < reducers)(lambda: sent_shares(reducers - 1))
            if reducers < n_seq:
                pl.when(seq >= reducers)(lambda: sent_shares(reducers))
            near = jnp.logical_and(seq // owners == block, origin == head)
            pl.when(jnp.logical_and(seq < reducers, jnp.logical_not(near)))(lambda: sent_finals(owners))
            if owners > 1:
                pl.when(jnp.logical_and(seq < reducers, near))(lambda: sent_finals(owners - 1))

        for origin in range(n_head):
            drain(origin, head, origin, 0)
        if helps:
            for way in range(2):
                for origin in range(n_head):
                    @pl.when(jnp.logical_and(helper(way), origin != block_of(way)))
                    def _():
                        drain(n_head + origin, block_of(way), origin, 1)


def finish(attn_ref, grad_ref, attn_out, grad_out, turned_ref, sem):
    attn_copy = pltpu.make_async_copy(attn_ref, attn_out, sem.at[0])
    attn_copy.start()
    turned_ref[...] = grad_ref[...].T
    grad_copy = pltpu.make_async_copy(turned_ref, grad_out, sem.at[1])
    grad_copy.start()
    attn_copy.wait()
    grad_copy.wait()


def body(n_seq, n_head, queries, keys, values, level_ids, level_table, out_cotangent):
    block_len, head_dim = queries.shape
    width = out_cotangent.shape[1]
    per = width * n_head // n_seq
    piece = per if per % 128 == 0 else width
    seq_bits = n_seq.bit_length() - 1
    tiles = block_len // TILE
    inner = tiles.bit_length() - 1
    rows_per = max(16, head_dim // n_seq)
    slots = 2 * n_head
    spare = max(4, tiles - kept_tiles(n_head, tiles))
    dma = pltpu.SemaphoreType.DMA
    vmem = pl.BlockSpec(memory_space=pltpu.VMEM)
    hbm = pl.BlockSpec(memory_space=pltpu.HBM)
    attn_out, grad = pl.pallas_call(
        functools.partial(kernel, n_seq, n_head),
        out_shape=(
            pltpu.VMEM((block_len, head_dim), BF16),
            pltpu.VMEM((head_dim, per), F32),
        ),
        in_specs=[hbm] * 6,
        out_specs=(vmem, vmem),
        scratch_shapes=[
            pltpu.VMEM((block_len, head_dim), BF16),
            pltpu.VMEM((block_len, head_dim), BF16),
            pltpu.VMEM((block_len, head_dim), BF16),
            pltpu.VMEM((block_len, width), BF16),
            pltpu.VMEM((1, block_len), jnp.int32),
            pltpu.VMEM(level_table.shape[::-1], F32),
            pltpu.VMEM((TILE, TILE), jnp.int32),
            pltpu.VMEM((block_len, level_table.shape[1]), F32),
            pltpu.VMEM((block_len, head_dim), F32),
            pltpu.VMEM((tiles, head_dim, inner * head_dim), BF16),
            pltpu.VMEM((head_dim, head_dim), BF16),
            pltpu.VMEM((n_seq, head_dim, head_dim), BF16),
            pltpu.VMEM((2 * head_dim, seq_bits * head_dim), BF16),
            pltpu.VMEM((n_head, tiles, head_dim, TILE), BF16),
            pltpu.VMEM((slots, head_dim, width), F32),
            pltpu.VMEM((slots, head_dim, width), BF16),
            pltpu.VMEM((slots, n_seq - 1, rows_per, width), BF16),
            pltpu.VMEM((slots, rows_per, width), BF16),
            pltpu.VMEM((2, head_dim, piece), BF16),
            pltpu.VMEM((head_dim, piece), F32),
            pltpu.VMEM((spare * TILE, width), BF16),
            dma((6,)),
            dma((1,)),
            dma((1,)),
            dma((2,)),
            dma((max(1, n_head - 1), tiles)),
            dma((slots,)),
            dma((slots,)),
            dma((slots,)),
            dma((2,)),
            dma((1,)),
            dma((1,)),
        ],
        compiler_params=pltpu.CompilerParams(
            collective_id=0, has_side_effects=True, vmem_limit_bytes=60 * 2**20
        ),
    )(queries, keys, values, level_ids[None, :], level_table.T, out_cotangent)
    return pl.pallas_call(
        finish,
        out_shape=(
            jax.ShapeDtypeStruct((block_len, head_dim), BF16),
            jax.ShapeDtypeStruct((per, head_dim), F32),
        ),
        in_specs=[vmem, vmem],
        out_specs=(hbm, hbm),
        scratch_shapes=[pltpu.VMEM((per, head_dim), F32), dma((2,))],
        compiler_params=pltpu.CompilerParams(vmem_limit_bytes=4 * 2**20),
    )(attn_out, grad)


def solution(mesh):
    in_specs = (
        P("seq", "head"),
        P("seq", "head"),
        P("seq", "head"),
        P("seq"),
        P(),
        P("seq", "head"),
    )
    out_specs = (P("seq", "head"), P("seq", "head"))
    return jax.shard_map(
        functools.partial(body, mesh.shape["seq"], mesh.shape["head"]),
        mesh=mesh, in_specs=in_specs, out_specs=out_specs, check_vma=False,
    )
```

```python
import functools

import jax
import jax.numpy as jnp
from jax import lax
from jax.experimental import pallas as pl
from jax.experimental.pallas import tpu as pltpu
from jax.sharding import PartitionSpec as P

EPSILON = 1e-06
TILE = 128
KEEP = 11
AHEAD = 8
LEAD = 6
LAG = 6
SETTLED = 12
BURST = 2
MESH = pl.DeviceIdType.MESH
F32 = jnp.float32
BF16 = jnp.bfloat16


def dot(a, b, ca, cb):
    return lax.dot_general(a, b, (((ca,), (cb,)), ((), ())), preferred_element_type=F32)


def tile_levels(tile):
    row = lax.broadcasted_iota(jnp.int32, (tile, tile), 0)
    col = lax.broadcasted_iota(jnp.int32, (tile, tile), 1)
    apart = jnp.bitwise_xor(row, col)
    levels = jnp.zeros((tile, tile), jnp.int32)
    for bit in range(tile.bit_length() - 1):
        levels = levels + (jnp.right_shift(apart, bit) > 0).astype(jnp.int32)
    return jnp.where(col <= row, levels, -1)


def kept_tiles(n_head, tiles):
    return tiles * KEEP // 16 if n_head >= 4 else tiles


def kernel(
    n_seq, n_head,
    q_hbm, k_hbm, v_hbm, ids_hbm, table_hbm, cot_hbm,
    attn_ref, grad_ref,
    q_ref, k_ref, v_ref, cot_ref, ids_ref, table_ref, levels_ref, coeff_ref, total_ref, sib_ref,
    state_ref, states_ref, flat_ref, gather_ref, acc_ref,
    share_ref, shares_ref, final_ref, finals_ref, whole_ref, help_ref,
    load_sem, state_send, state_recv, ring_send, ring_recv,
    share_send, share_recv, final_send, final_recv, help_send, help_recv,
):
    seq, head = lax.axis_index("seq"), lax.axis_index("head")
    block_len, head_dim = q_ref.shape
    width = cot_ref.shape[1]
    tiles = block_len // TILE
    pairs = tiles // 2
    tile_bits = TILE.bit_length() - 1
    local_bits = block_len.bit_length() - 1
    inner = local_bits - tile_bits
    seq_bits = n_seq.bit_length() - 1
    owners = n_seq // n_head
    rows_per = max(16, head_dim // n_seq)
    reducers = head_dim // rows_per
    piece = finals_ref.shape[2]
    last = n_head - 1
    keep = kept_tiles(n_head, tiles)
    helps = keep < tiles
    quads = tiles // 4
    ahead = min(AHEAD, tiles)
    lead = min(LEAD, ahead)
    scale = (block_len * n_seq) ** (-0.5)

    loads = [
        pltpu.make_async_copy(src, dst, load_sem.at[i])
        for i, (src, dst) in enumerate(
            [
                (k_hbm, k_ref), (v_hbm, v_ref), (table_hbm, table_ref), (ids_hbm, ids_ref),
                (q_hbm, q_ref), (cot_hbm, cot_ref),
            ]
        )
    ]
    for load in loads[:4]:
        load.start()

    barrier = pltpu.get_barrier_semaphore()

    def greet(device):
        pl.semaphore_signal(barrier, inc=1, device_id=device, device_id_type=MESH)

    for step in range(1, n_seq):
        greet((lax.rem(seq + step, n_seq), head))
    pl.when(head > 0)(lambda: greet((seq, head - 1)))
    pl.when(head < n_head - 1)(lambda: greet((seq, head + 1)))

    levels_ref[...] = tile_levels(TILE)
    right, left = lax.rem(head + 1, n_head), lax.rem(head + n_head - 1, n_head)
    neighbours = (right, left)
    places = (head, last - head)

    half = n_head // 2
    spare = tiles - keep

    def origin_of(way, distance):
        return head - distance if way == 0 else head + distance

    def upward(origin):
        inside = jnp.logical_and(origin > 0, origin < half)
        return jnp.logical_or(inside, origin == last)

    def tile_of(origin, i):
        return jnp.where(upward(origin), i, tiles - 1 - i)

    def quad_of(origin, j):
        return jnp.where(upward(origin), j, quads - 1 - j)

    def kept(way, c):
        return c >= spare if way == 0 else c < keep

    def kept_quad(way, q):
        return 4 * q + 3 >= spare if way == 0 else 4 * q < keep

    def help_copy(way, i):
        return pltpu.make_async_remote_copy(
            src_ref=cot_hbm.at[pl.ds(i * TILE if way == 0 else (keep + i) * TILE, TILE), :],
            dst_ref=help_ref.at[pl.ds(i * TILE, TILE), :],
            send_sem=help_send.at[0], recv_sem=help_recv.at[0],
            device_id=(seq, left if way == 0 else right), device_id_type=MESH,
        )

    at_edge = jnp.logical_or(head == 0, head == last)

    def meet():
        pl.semaphore_wait(barrier, n_seq - 1 + jnp.minimum(head, 1) + jnp.minimum(last - head, 1))

    @pl.when(at_edge)
    def _():
        meet()
        for way in range(2):
            @pl.when(places[way] == last)
            def _():
                for i in range(spare):
                    help_copy(way, i).start()

    with jax.named_scope("kv"):
        for load in loads[:4]:
            load.wait()
    for load in loads[4:]:
        load.start()
    table = table_ref[...]
    high = table.astype(BF16)
    rest = table - high.astype(F32)
    mid = rest.astype(BF16)
    low = (rest - mid.astype(F32)).astype(BF16)
    table3 = jnp.concatenate([high, mid, low], axis=1)

    nodes = [
        dot(k_ref[pl.ds(i * TILE, TILE), :], v_ref[pl.ds(i * TILE, TILE), :], 0, 0)
        for i in range(tiles)
    ]
    for bit in range(inner):
        for i in range(tiles):
            place = (i >> bit) ^ 1
            value = nodes[place].astype(BF16) if (i >> bit) & 1 else jnp.zeros((head_dim, head_dim), BF16)
            sib_ref[i, :, pl.ds(bit * head_dim, head_dim)] = value
        nodes = [nodes[2 * i] + nodes[2 * i + 1] for i in range(len(nodes) // 2)]
    state_ref[...] = nodes[0].astype(BF16)


    def local_tile(i):
        rows = pl.ds(pl.multiple_of(i * TILE, TILE), TILE)
        row_ids = lax.broadcasted_iota(jnp.int32, (table.shape[1], TILE), 0)
        onehot = (row_ids == ids_ref[:, rows]).astype(F32).astype(BF16)
        coeff = dot(jnp.concatenate([onehot] * 3, axis=0), table3, 0, 1)
        coeff_ref[rows, :] = coeff
        levels = levels_ref[...]
        weights = jnp.zeros((TILE, TILE), F32)
        for level in range(tile_bits + 1):
            weights = jnp.where(levels == level, coeff[:, level : level + 1], weights)
        query = q_ref[rows, :]
        scores = dot(query, k_ref[rows, :], 1, 1)
        total = dot((weights * scores).astype(BF16), v_ref[rows, :], 1, 0)
        readout = dot(query, sib_ref[i], 1, 0)
        for bit in range(inner):
            level = tile_bits + 1 + bit
            total += coeff[:, level : level + 1] * readout[:, bit * head_dim : (bit + 1) * head_dim]
        total_ref[rows, :] = total

    def local_tiles(start, stop):
        def one(i, carry):
            local_tile(tile_of(head, i))
            return carry

        lax.fori_loop(start, stop, one, 0, unroll=True)

    with jax.named_scope("barrier"):
        pl.when(jnp.logical_not(at_edge))(meet)

    def state_copy(target):
        return pltpu.make_async_remote_copy(
            src_ref=state_ref, dst_ref=states_ref.at[seq],
            send_sem=state_send.at[0], recv_sem=state_recv.at[0],
            device_id=(target, head), device_id_type=MESH,
        )

    def partner(k):
        place = 0
        for bit in range(seq_bits):
            mine = lax.rem(seq // 2**bit, 2)
            place += 2**bit * (1 - mine if (k >> bit) & 1 else mine)
        return place

    for k in range(n_seq - 1, 0, -1):
        @pl.when(seq < partner(k))
        def _():
            state_copy(partner(k)).start()

    loads[4].wait()
    with jax.named_scope("local1"):
        local_tiles(0, ahead)
    acc_ref[...] = jnp.zeros_like(acc_ref)
    for way in range(2):
        blank = range(spare // 4 * 4, spare) if way == 0 else range(keep, (keep + 3) // 4 * 4)

        @pl.when(places[way] == last)
        def _():
            for c in blank:
                for origin in range(n_head):
                    @pl.when(origin != head)
                    def _():
                        gather_ref[origin, c] = jnp.zeros((head_dim, TILE), BF16)

    with jax.named_scope("states"):
        for block in range(1, n_seq):
            @pl.when(seq == block)
            def _():
                arrived = states_ref.at[pl.ds(0, block)]
                pltpu.make_async_remote_copy(
                    src_ref=arrived, dst_ref=arrived,
                    send_sem=state_send.at[0], recv_sem=state_recv.at[0],
                    device_id=(0, head), device_id_type=MESH,
                ).wait_recv()

    for bit in range(seq_bits):
        span = 2**bit
        node = seq // span
        columns = pl.ds(bit * head_dim, head_dim)

        @pl.when(lax.rem(node, 2) == 1)
        def _():
            total = jnp.zeros((head_dim, head_dim), F32)
            for offset in range(span):
                total += states_ref[(node - 1) * span + offset].astype(F32)
            upper = total.astype(BF16)
            flat_ref[pl.ds(0, head_dim), columns] = upper
            flat_ref[pl.ds(head_dim, head_dim), columns] = (total - upper.astype(F32)).astype(BF16)

        @pl.when(lax.rem(node, 2) == 0)
        def _():
            flat_ref[:, columns] = jnp.zeros((2 * head_dim, head_dim), BF16)

    def ring_copy(way, origin, c):
        return pltpu.make_async_remote_copy(
            src_ref=gather_ref.at[origin, c], dst_ref=gather_ref.at[origin, c],
            send_sem=ring_send.at[way], recv_sem=ring_recv.at[origin - way, c],
            device_id=(seq, neighbours[way]), device_id_type=MESH,
        )

    def passes(way, c):
        place = places[way]
        return jnp.logical_or(place + 1 < last, jnp.logical_and(place < last, kept(way, c)))

    def relay(way, distance, i):
        origin = origin_of(way, distance)
        c = tile_of(origin, i)
        ring_copy(way, origin, c).wait_recv()

        @pl.when(passes(way, c))
        def _():
            ring_copy(way, origin, c).start()

    def attn_tile(i):
        rows = pl.ds(pl.multiple_of(i * TILE, TILE), TILE)
        query = q_ref[rows, :]
        readout = dot(jnp.concatenate([query, query], axis=1), flat_ref[...], 1, 0)
        coeff = coeff_ref[rows, :]
        cross = jnp.zeros((TILE, head_dim), F32)
        for bit in range(seq_bits):
            level = local_bits + 1 + bit
            cross += coeff[:, level : level + 1] * readout[:, bit * head_dim : (bit + 1) * head_dim]
        total = total_ref[rows, :] + cross
        normed = total * lax.rsqrt(jnp.mean(total * total, axis=1, keepdims=True) + EPSILON)
        attn_ref[rows, :] = normed.astype(BF16)
        gather_ref[head, i] = normed.T.astype(BF16)

    def middle(way):
        return jnp.logical_and(places[way] >= 2, places[way] < last)

    early_tiles = BURST * spare

    def produce(local, relaying):
        def step(t, carry):
            tile = tile_of(head, t)
            attn_tile(tile)
            if local:
                local_tile(tile_of(head, t + ahead - lead))
            for way in range(2):
                @pl.when(passes(way, tile))
                def _():
                    ring_copy(way, head, tile).start()
            if relaying:
                for way in range(2):
                    @pl.when(jnp.logical_and(middle(way), t >= keep))
                    def _():
                        for i in range(BURST):
                            relay(way, 1, BURST * (t - keep) + i)
            return carry
        return step

    with jax.named_scope("phase1o"):
        lax.fori_loop(0, lead, produce(False, False), 0)
    with jax.named_scope("phase1a"):
        lax.fori_loop(lead, tiles - ahead + lead, produce(True, True), 0)
    with jax.named_scope("phase1b"):
        lax.fori_loop(tiles - ahead + lead, tiles, produce(False, True), 0)

    def joined(origin, q):
        return jnp.concatenate([gather_ref[origin, 4 * q + i] for i in range(4)], axis=1)

    def multiply(origin, q):
        rows = pl.ds(pl.multiple_of(q * (4 * TILE), 4 * TILE), 4 * TILE)
        acc_ref[origin] += dot(joined(origin, q), cot_ref[rows, :], 1, 0)

    def multiply_help(way, origin):
        base = 0 if way == 0 else keep
        for start in range(0, spare, 4):
            group = range(start, min(start + 4, spare))
            block = jnp.concatenate([gather_ref[origin, base + i] for i in group], axis=1)
            rows = help_ref[start * TILE : (group[-1] + 1) * TILE, :]
            acc_ref[n_head + origin] += dot(block, rows, 1, 0)

    def share_copy(slot, k):
        target = partner(k)
        return pltpu.make_async_remote_copy(
            src_ref=share_ref.at[slot, pl.ds(pl.multiple_of(target * rows_per, rows_per), rows_per), :],
            dst_ref=shares_ref.at[slot, k - 1],
            send_sem=share_send.at[slot], recv_sem=share_recv.at[slot],
            device_id=(target, head), device_id_type=MESH,
        )

    def send_share(slot):
        share_ref[slot] = (acc_ref[slot] * scale).astype(BF16)
        for k in range(n_seq - 1, 0, -1):
            if reducers == n_seq:
                share_copy(slot, k).start()
            else:
                pl.when(partner(k) < reducers)(lambda: share_copy(slot, k).start())

    def final_copy(slot, block, origin, kind, owner):
        columns = pl.ds(owner * piece if piece < width else 0, piece)
        return pltpu.make_async_remote_copy(
            src_ref=final_ref.at[slot, :, columns] if piece < width else final_ref.at[slot],
            dst_ref=finals_ref.at[kind, pl.ds(pl.multiple_of(seq * rows_per, rows_per), rows_per), :],
            send_sem=final_send.at[slot], recv_sem=final_recv.at[kind],
            device_id=(block * owners + owner, origin), device_id_type=MESH,
        )

    def is_self(block, origin, owner):
        return jnp.logical_and(block * owners + owner == seq, origin == head)

    def reduce_share(slot, block, origin, kind):
        @pl.when(seq < reducers)
        def _():
            mine = pl.ds(pl.multiple_of(seq * rows_per, rows_per), rows_per)
            arrived = shares_ref.at[slot]
            pltpu.make_async_remote_copy(
                src_ref=arrived, dst_ref=arrived,
                send_sem=share_send.at[slot], recv_sem=share_recv.at[slot],
                device_id=(0, head), device_id_type=MESH,
            ).wait_recv()
            whole = acc_ref[slot, mine, :] * scale
            for source in range(n_seq - 1):
                whole += shares_ref[slot, source].astype(F32)
            final_ref[slot] = whole.astype(BF16)
            for owner in range(owners):
                @pl.when(jnp.logical_not(is_self(block, origin, owner)))
                def _():
                    final_copy(slot, block, origin, kind, owner).start()

                @pl.when(is_self(block, origin, owner))
                def _():
                    start = owner * piece if piece < width else 0
                    finals_ref[kind, mine, :] = final_ref[slot, :, pl.ds(start, piece)]

    loads[5].wait()

    def arrive(way, origin, q):
        for c in range(4):
            @pl.when(kept(way, 4 * q + c))
            def _():
                ring_copy(way, origin, 4 * q + c).wait_recv()

    def helper(way):
        return jnp.logical_and(places[way] == last - 1, helps)

    def block_of(way):
        return last if way == 0 else 0

    def every_group(distance, act):
        @pl.when(distance == 0)
        def _():
            act(head, head, head, 0)
            if helps:
                for way in range(2):
                    pl.when(helper(way))(functools.partial(act, n_head + head, block_of(way), head, 1))

        for way in range(2):
            origin = origin_of(way, distance)

            @pl.when(jnp.logical_and(distance > 0, distance < places[way]))
            def _():
                act(origin, head, origin, 0)
                if helps:
                    pl.when(helper(way))(functools.partial(act, n_head + origin, block_of(way), origin, 1))

    began = early_tiles
    if last > 3:
        began = tiles
        for way in range(2):
            def rest(i, carry):
                relay(way, 1, i)
                return carry

            def more(n, carry):
                relay(way, 2 + n // tiles, lax.rem(n, tiles))
                return carry

            @pl.when(middle(way))
            def _():
                lax.fori_loop(early_tiles, tiles, rest, 0)
                lax.fori_loop(0, (places[way] - 2) * tiles, more, 0)

    farthest = jnp.maximum(places[0], places[1])

    def flow(u, carry):
        for way in range(2):
            place, origin = places[way], block_of(1 - way)
            i = u - 1 - LAG * (place - 1)

            if began < tiles:
                @pl.when(jnp.logical_and(middle(way), u < tiles - began))
                def _():
                    relay(way, 1, began + u)

            @pl.when(jnp.logical_and(jnp.logical_and(place > 0, place < last), jnp.logical_and(i >= 0, i < tiles)))
            def _():
                relay(way, place, i)

        for way in range(2):
            place, origin = places[way], block_of(1 - way)
            i = u - 1 - LAG * (place - 1)
            j = i // 4
            q = quad_of(origin, j)

            @pl.when(jnp.logical_and(jnp.logical_and(place > 0, i - 4 * j == 3), jnp.logical_and(i >= 0, i < tiles)))
            def _():
                @pl.when(jnp.logical_or(place < last, kept_quad(way, q)))
                def _():
                    pl.when(place == last)(functools.partial(arrive, way, origin, q))
                    multiply(origin, q)
                done = jnp.where(place == last, (keep + 3) // 4 - 1, quads - 1)
                pl.when(j == done)(functools.partial(send_share, origin))
                if helps:
                    @pl.when(jnp.logical_and(helper(way), j == quads - 1))
                    def _():
                        multiply_help(way, origin)
                        send_share(n_head + origin)

        distance = u // quads
        j = u - quads * distance

        @pl.when(distance == 0)
        def _():
            multiply(head, quad_of(head, j))

        for way in range(2):
            place, origin = places[way], origin_of(way, distance)
            q = quad_of(origin, j)

            @pl.when(jnp.logical_and(jnp.logical_and(distance > 0, distance < place), jnp.logical_or(place < last, kept_quad(way, q))))
            def _():
                pl.when(place == last)(functools.partial(arrive, way, origin, q))
                multiply(origin, q)

            if helps:
                @pl.when(jnp.logical_and(helper(way), jnp.logical_and(distance < place, j == quads - 1)))
                def _():
                    @pl.when(distance == 0)
                    def _():
                        pltpu.make_async_remote_copy(
                            src_ref=help_ref, dst_ref=help_ref,
                            send_sem=help_send.at[0], recv_sem=help_recv.at[0],
                            device_id=(seq, left if way == 0 else right), device_id_type=MESH,
                        ).wait_recv()
                    multiply_help(way, origin)

        @pl.when(j == quads - 1)
        def _():
            every_group(distance, lambda slot, *_: send_share(slot))

        behind = jnp.maximum(u - SETTLED, 0)

        @pl.when(jnp.logical_and(jnp.logical_and(u >= SETTLED, lax.rem(behind, quads) == 0), behind // quads < farthest))
        def _():
            every_group(behind // quads, reduce_share)
        return carry

    with jax.named_scope("flow"):
        lax.fori_loop(0, jnp.maximum(tiles + 1 + LAG * (farthest - 1), quads * (farthest - 1) + SETTLED + 1), flow, 0)

    ends = []
    for way in range(2):
        place, origin = places[way], block_of(1 - way)
        if helps:
            ends.append((helper(way), n_head + origin, block_of(way), origin, 1))
    for way in range(2):
        place, origin = places[way], block_of(1 - way)
        ends.append((place > 0, origin, head, origin, 0))
    with jax.named_scope("reducelast"):
        closer = places[0] <= places[1]
        nearer = (closer, jnp.logical_not(closer))

        def reduce_main(flip):
            for turn, (condition, *rest) in zip(flip, ends[-2:]):
                pl.when(jnp.logical_and(turn, condition))(functools.partial(reduce_share, *rest))

        reduce_main(nearer)
        for condition, *rest in ends[:-2]:
            pl.when(condition)(functools.partial(reduce_share, *rest))
        reduce_main(nearer[::-1])

    with jax.named_scope("finals"):
        home = seq // owners
        at_end = jnp.logical_and(jnp.logical_or(home == 0, home == last), head != home)
        for kind in range(2 if helps else 1):
            plane = home if kind == 0 else jnp.where(home == 0, 1, last - 1)
            own = jnp.logical_and(seq < reducers, head == plane)
            expected = at_end if kind else seq >= 0
            for count, match in ((reducers - 1, own), (reducers, jnp.logical_not(own))):
                @pl.when(jnp.logical_and(expected, match))
                def _():
                    arrived = finals_ref.at[kind, pl.ds(0, count * rows_per), :]
                    pltpu.make_async_remote_copy(
                        src_ref=arrived, dst_ref=arrived,
                        send_sem=final_send.at[0], recv_sem=final_recv.at[kind],
                        device_id=(0, plane), device_id_type=MESH,
                    ).wait_recv()
        whole_ref[...] = finals_ref[0].astype(F32)
        if helps:
            @pl.when(at_end)
            def _():
                whole_ref[...] += finals_ref[1].astype(F32)
        per = grad_ref.shape[1]
        if per == piece:
            grad_ref[...] = whole_ref[...]
        else:
            for owner in range(owners):
                @pl.when(lax.rem(seq, owners) == owner)
                def _():
                    grad_ref[...] = whole_ref[:, owner * per : (owner + 1) * per]

    with jax.named_scope("drain"):
        for block in range(n_seq - 1):
            @pl.when(seq == block)
            def _():
                sent = states_ref.at[pl.ds(0, n_seq - 1 - block)]
                pltpu.make_async_remote_copy(
                    src_ref=sent, dst_ref=sent,
                    send_sem=state_send.at[0], recv_sem=state_recv.at[0],
                    device_id=(0, head), device_id_type=MESH,
                ).wait_send()
        for way in range(2):
            if helps:
                @pl.when(places[way] == last)
                def _():
                    pltpu.make_async_remote_copy(
                        src_ref=help_ref, dst_ref=help_ref,
                        send_sem=help_send.at[0], recv_sem=help_recv.at[0],
                        device_id=(seq, left if way == 0 else right), device_id_type=MESH,
                    ).wait_send()
            for place in range(last):
                @pl.when(places[way] == place)
                def _():
                    count = tiles if place + 1 < last else keep
                    sent = gather_ref.at[pl.ds(0, place + 1), pl.ds(0, count)]
                    pltpu.make_async_remote_copy(
                        src_ref=sent, dst_ref=sent,
                        send_sem=ring_send.at[way], recv_sem=ring_recv.at[0, 0],
                        device_id=(seq, neighbours[way]), device_id_type=MESH,
                    ).wait_send()
        def drain(slot, block, origin, kind):
            def sent_shares(count):
                sent = share_ref.at[slot, pl.ds(0, count * rows_per), :]
                pltpu.make_async_remote_copy(
                    src_ref=sent, dst_ref=sent,
                    send_sem=share_send.at[slot], recv_sem=share_recv.at[slot],
                    device_id=(0, head), device_id_type=MESH,
                ).wait_send()

            def sent_finals(count):
                sent = finals_ref.at[0, pl.ds(0, count * rows_per), :]
                pltpu.make_async_remote_copy(
                    src_ref=sent, dst_ref=sent,
                    send_sem=final_send.at[slot], recv_sem=final_recv.at[0],
                    device_id=(0, head), device_id_type=MESH,
                ).wait_send()

            pl.when(seq < reducers)(lambda: sent_shares(reducers - 1))
            if reducers < n_seq:
                pl.when(seq >= reducers)(lambda: sent_shares(reducers))
            near = jnp.logical_and(seq // owners == block, origin == head)
            pl.when(jnp.logical_and(seq < reducers, jnp.logical_not(near)))(lambda: sent_finals(owners))
            if owners > 1:
                pl.when(jnp.logical_and(seq < reducers, near))(lambda: sent_finals(owners - 1))

        for origin in range(n_head):
            drain(origin, head, origin, 0)
        if helps:
            for way in range(2):
                for origin in range(n_head):
                    @pl.when(jnp.logical_and(helper(way), origin != block_of(way)))
                    def _():
                        drain(n_head + origin, block_of(way), origin, 1)


def finish(attn_ref, grad_ref, attn_out, grad_out, turned_ref, sem):
    attn_copy = pltpu.make_async_copy(attn_ref, attn_out, sem.at[0])
    attn_copy.start()
    turned_ref[...] = grad_ref[...].T
    grad_copy = pltpu.make_async_copy(turned_ref, grad_out, sem.at[1])
    grad_copy.start()
    attn_copy.wait()
    grad_copy.wait()


def body(n_seq, n_head, queries, keys, values, level_ids, level_table, out_cotangent):
    block_len, head_dim = queries.shape
    width = out_cotangent.shape[1]
    per = width * n_head // n_seq
    piece = per if per % 128 == 0 else width
    seq_bits = n_seq.bit_length() - 1
    tiles = block_len // TILE
    inner = tiles.bit_length() - 1
    rows_per = max(16, head_dim // n_seq)
    slots = 2 * n_head
    spare = max(4, tiles - kept_tiles(n_head, tiles))
    dma = pltpu.SemaphoreType.DMA
    vmem = pl.BlockSpec(memory_space=pltpu.VMEM)
    hbm = pl.BlockSpec(memory_space=pltpu.HBM)
    attn_out, grad = pl.pallas_call(
        functools.partial(kernel, n_seq, n_head),
        out_shape=(
            pltpu.VMEM((block_len, head_dim), BF16),
            pltpu.VMEM((head_dim, per), F32),
        ),
        in_specs=[hbm] * 6,
        out_specs=(vmem, vmem),
        scratch_shapes=[
            pltpu.VMEM((block_len, head_dim), BF16),
            pltpu.VMEM((block_len, head_dim), BF16),
            pltpu.VMEM((block_len, head_dim), BF16),
            pltpu.VMEM((block_len, width), BF16),
            pltpu.VMEM((1, block_len), jnp.int32),
            pltpu.VMEM(level_table.shape[::-1], F32),
            pltpu.VMEM((TILE, TILE), jnp.int32),
            pltpu.VMEM((block_len, level_table.shape[1]), F32),
            pltpu.VMEM((block_len, head_dim), F32),
            pltpu.VMEM((tiles, head_dim, inner * head_dim), BF16),
            pltpu.VMEM((head_dim, head_dim), BF16),
            pltpu.VMEM((n_seq, head_dim, head_dim), BF16),
            pltpu.VMEM((2 * head_dim, seq_bits * head_dim), BF16),
            pltpu.VMEM((n_head, tiles, head_dim, TILE), BF16),
            pltpu.VMEM((slots, head_dim, width), F32),
            pltpu.VMEM((slots, head_dim, width), BF16),
            pltpu.VMEM((slots, n_seq - 1, rows_per, width), BF16),
            pltpu.VMEM((slots, rows_per, width), BF16),
            pltpu.VMEM((2, head_dim, piece), BF16),
            pltpu.VMEM((head_dim, piece), F32),
            pltpu.VMEM((spare * TILE, width), BF16),
            dma((6,)),
            dma((1,)),
            dma((1,)),
            dma((2,)),
            dma((max(1, n_head - 1), tiles)),
            dma((slots,)),
            dma((slots,)),
            dma((slots,)),
            dma((2,)),
            dma((1,)),
            dma((1,)),
        ],
        compiler_params=pltpu.CompilerParams(
            collective_id=0, has_side_effects=True, vmem_limit_bytes=60 * 2**20
        ),
    )(queries, keys, values, level_ids[None, :], level_table.T, out_cotangent)
    return pl.pallas_call(
        finish,
        out_shape=(
            jax.ShapeDtypeStruct((block_len, head_dim), BF16),
            jax.ShapeDtypeStruct((per, head_dim), F32),
        ),
        in_specs=[vmem, vmem],
        out_specs=(hbm, hbm),
        scratch_shapes=[pltpu.VMEM((per, head_dim), F32), dma((2,))],
        compiler_params=pltpu.CompilerParams(vmem_limit_bytes=4 * 2**20),
    )(attn_out, grad)


def solution(mesh):
    in_specs = (
        P("seq", "head"),
        P("seq", "head"),
        P("seq", "head"),
        P("seq"),
        P(),
        P("seq", "head"),
    )
    out_specs = (P("seq", "head"), P("seq", "head"))
    return jax.shard_map(
        functools.partial(body, mesh.shape["seq"], mesh.shape["head"]),
        mesh=mesh, in_specs=in_specs, out_specs=out_specs, check_vma=False,
    )
```
